32 devices in a mesh: gx: 4 (over x, core), gy: 8 (over z, y).
Axes of the slice: x: 2, y: 2, z: 4, core: 2. Of those that a mesh axis runs over, the one named last changes fastest.
Arguments:
- fine_start: float32 [3, 1024, 4096], P(None, 'gx', 'gy'), may hold values from -6 to 6
- fine_known: float32 [3, 1024, 4096], P(None, 'gx', 'gy'), may hold values from -18 to 18
- fine_mu: float32 [1024, 4096], P('gx', 'gy'), may hold values from 1 to 10
- coarse_start: float32 [3, 512, 2048], P(None, ('gx', 'gy')), may hold values from -6 to 6
- coarse_known: float32 [3, 512, 2048], P(None, ('gx', 'gy')), may hold values from -18 to 18
- coarse_mu: float32 [512, 2048], P(('gx', 'gy')), may hold values from 1 to 10
Outputs:
- fine_ghost: float32 [3, 1024, 4096], P(None, 'gx', 'gy')
- coarse_ghost: float32 [3, 512, 2048], P(None, ('gx', 'gy'))
- norms: float32 [3], replicated
The draws below stay inside these ranges and needn't reach their ends.
All inputs are finite; a program needn't handle non-finite values.
Results may differ from the reference program's by a relative error of at most 0.0001.
Values sent between devices are 32-bit elements; how exact they have to be, the bound alone decides.
A program may use at most 128 MiB of HBM per device.

```python
import math
import jax
import jax.numpy as jnp

ITERS = 3
NCX = 512
NCY = 2048
NFX = 1024
NFY = 4096


def rising_field(key, rows, cols):
    ramp = 1.0 + 2.0 * jnp.arange(rows, dtype=jnp.float32)[:, None] / max(rows - 1, 1)
    base = jnp.clip(jax.random.normal(key, (3, rows, cols), jnp.float32), -6.0, 6.0)
    return base * ramp[None]


def draw_fine_known(key, part):
    return rising_field(jax.random.fold_in(key, 11), NFX, NFY)


def draw_coarse_known(key, part):
    return rising_field(jax.random.fold_in(key, 23), NCX, NCY)


def steps_of(stream_key, extent, split, least, top_value):
    def one(dim, blocks):
        steps = jax.random.uniform(jax.random.fold_in(jax.random.fold_in(stream_key, 6), dim), (blocks,), jnp.float32, least / len(split), top_value / len(split))
        return jnp.repeat(jnp.exp(steps), extent[dim] // blocks).reshape((-1,) + (1,) * (len(extent) - dim - 1))

    gain = one(*split[0])
    for cut in split[1:]:
        gain = gain * one(*cut)
    return gain


def bell_draw(key, extent, spread, limit, split=(), kind=jnp.bfloat16):
    factor_of = steps_of(key, extent, split, -0.22, 0.18) if split else 1.0
    drawn = jax.random.normal(key, extent, jnp.float32) * spread * factor_of
    return jnp.minimum(jnp.maximum(drawn, -limit), limit).astype(kind)


def setup_inputs(seed: int = 0) -> dict:
    arg_keys = jax.random.split(jax.random.key(seed), 7)
    return {
        "fine_start": bell_draw(arg_keys[0], (3, NFX, NFY), 1.0, 6.0, ((1, 4), (2, 8)), jnp.float32),
        "fine_known": draw_fine_known(jax.random.fold_in(arg_keys[6], 71), 0),
        "fine_mu": jnp.clip(jnp.exp(math.log(10.0) - 2.3025851 * jax.random.uniform(arg_keys[2], (NFX, NFY), jnp.float32) ** steps_of(arg_keys[2], (NFX, NFY), ((0, 4), (1, 8)), -0.2, 0.2)), 1.0, 10.0),
        "coarse_start": bell_draw(arg_keys[3], (3, NCX, NCY), 1.0, 6.0, ((1, 32),), jnp.float32),
        "coarse_known": draw_coarse_known(jax.random.fold_in(arg_keys[6], 71), 0),
        "coarse_mu": jnp.clip(jnp.exp(math.log(10.0) - 2.3025851 * jax.random.uniform(arg_keys[5], (NCX, NCY), jnp.float32) ** steps_of(arg_keys[5], (NCX, NCY), ((0, 32),), -0.2, 0.2)), 1.0, 10.0),
    }


def neighbours(padded):
    return padded[:, 2:, 1:-1] + padded[:, :-2, 1:-1] + padded[:, 1:-1, 2:] + padded[:, 1:-1, :-2]

def prolong(padded):
    components, rows_plus, cols_plus = padded.shape
    middle = padded[:, 1:-1, :]
    even_rows = 0.75 * middle + 0.25 * padded[:, :-2, :]
    odd_rows = 0.75 * middle + 0.25 * padded[:, 2:, :]
    row_fine = jnp.stack([even_rows, odd_rows], axis=2).reshape(components, 2 * (rows_plus - 2), cols_plus)
    centre = row_fine[:, :, 1:-1]
    even_cols = 0.75 * centre + 0.25 * row_fine[:, :, :-2]
    odd_cols = 0.75 * centre + 0.25 * row_fine[:, :, 2:]
    return jnp.stack([even_cols, odd_cols], axis=3).reshape(components, 2 * (rows_plus - 2), 2 * (cols_plus - 2))

def restrict(fine):
    return 0.25 * (fine[:, 0::2, 0::2] + fine[:, 1::2, 0::2] + fine[:, 0::2, 1::2] + fine[:, 1::2, 1::2])

def pad_plane(field):
    return jnp.pad(field, ((0, 0), (1, 1), (1, 1)))

def reference(fine_start, fine_known, fine_mu, coarse_start, coarse_known, coarse_mu):
    fine_diag = (fine_mu + 1.0)[None]
    coarse_diag = (coarse_mu + 1.0)[None]
    fine_ghost = fine_start
    coarse_ghost = coarse_start
    cell_total = 3.0 * (NFX * NFY + NCX * NCY)
    norm_list = []
    for sweep in range(ITERS):
        coarse_padded = pad_plane(coarse_ghost)
        fine_res = fine_known + 0.25 * neighbours(pad_plane(fine_ghost)) + 0.5 * prolong(coarse_padded) - fine_diag * fine_ghost
        coarse_res = coarse_known + 0.25 * neighbours(coarse_padded) + 0.5 * restrict(fine_ghost) - coarse_diag * coarse_ghost
        total = jnp.sum(fine_res * fine_res) + jnp.sum(coarse_res * coarse_res)
        norm_list.append(jnp.sqrt(total / cell_total))
        fine_ghost = fine_ghost + fine_res / fine_diag
        coarse_ghost = coarse_ghost + coarse_res / coarse_diag
    return (fine_ghost, coarse_ghost, jnp.stack(norm_list))
```

```python
import functools

import jax
import jax.numpy as jnp
from jax import lax
from jax.experimental import pallas as pl
from jax.experimental.pallas import tpu as pltpu
from jax.sharding import PartitionSpec as P

ITERS = 3
LANES = 128
SUB = 8
HALF = LANES // 2
AHEAD_CENTRAL = 2
AHEAD_OUTER = 2
VMEM_BYTES = 67043328
MESH = pl.DeviceIdType.MESH
DIRECTIONS = ((-1, 0), (1, 0), (0, -1), (0, 1), (-1, -1), (1, 1), (-1, 1), (1, -1))


def lane_index():
    return lax.broadcasted_iota(jnp.int32, (SUB, LANES), 1)


def roll_lanes(cells, shift):
    shift = shift % LANES
    return cells if shift == 0 else pltpu.roll(cells, shift, 1)


def from_left(halves, halo):
    first = lane_index() == 0
    rolled = [roll_lanes(cells, 1) for cells in halves]
    return [jnp.where(first, before, own) for before, own in zip([halo] + rolled[:-1], rolled)]


def from_right(halves, halo):
    last = lane_index() == LANES - 1
    rolled = [roll_lanes(cells, LANES - 1) for cells in halves]
    return [jnp.where(last, after, own) for own, after in zip(rolled, rolled[1:] + [halo])]


def spread_rows(*rows):
    share = LANES // len(rows)
    return jnp.concatenate(
        [jnp.broadcast_to(row, (share, row.shape[1])) for row in rows], axis=0
    ).T


def kernel(
    n_gx,
    n_gy,
    cells_total,
    fine_start,
    fine_known,
    fine_mu,
    coarse_start,
    coarse_known,
    coarse_mu,
    fine_out,
    coarse_out,
    norms_out,
    raw_start,
    raw_known,
    raw_mu,
    fine_a,
    fine_b,
    known,
    diag,
    inverse,
    patch_start,
    patch_known,
    patch_mu,
    patch_inverse,
    coarse_a,
    coarse_b,
    patch_out,
    fine_row_send,
    fine_row_recv,
    fine_col_send,
    fine_col_recv,
    row_send,
    row_recv,
    col_send,
    col_recv,
    corner_recv,
    fine_halo,
    coarse_halo,
    norm_all,
    tally,
    load_sem,
    move_send,
    move_recv,
    fine_send,
    fine_recv,
    halo_send,
    halo_recv,
    back_send,
    back_recv,
    norm_send,
    norm_recv,
):
    gx = lax.axis_index("gx")
    gy = lax.axis_index("gy")
    me = gx * n_gy + gy
    count = n_gx * n_gy
    central = jnp.logical_and(4 * gy >= n_gy, 4 * gy < 3 * n_gy)
    fine, coarse = (fine_a, fine_b), (coarse_a, coarse_b)
    comps, rows, width = patch_start.shape
    halves = width // LANES
    tiles = 2 * halves
    blocks = rows // SUB
    own_rows = coarse_start.shape[1]
    lane = lane_index()
    barrier = pltpu.get_barrier_semaphore()

    def each_device(action):
        def along_gx(dx, carry):
            def along_gy(dy, inner_carry):
                action({"gx": lax.rem(gx + dx, n_gx), "gy": lax.rem(gy + dy, n_gy)})
                return inner_carry

            return lax.fori_loop(jnp.where(dx == 0, 1, 0), n_gy, along_gy, carry)

        lax.fori_loop(0, n_gx, along_gx, 0)

    each_device(
        lambda peer: pl.semaphore_signal(barrier, inc=1, device_id=peer, device_id_type=MESH)
    )

    loads = []
    for which, (source, target) in enumerate(
        ((fine_start, raw_start), (fine_mu, raw_mu), (fine_known, raw_known))
    ):
        for tile in range(tiles):
            at = pl.ds(tile * LANES, LANES)
            view = source.at[:, at] if len(source.shape) == 2 else source.at[:, :, at]
            loads.append(
                pltpu.make_async_copy(view, target.at[tile], load_sem.at[which])
            )
    for copy in loads:
        copy.start()

    def wait_bytes(ref, sem):
        pltpu.make_async_copy(ref, ref, sem).wait()

    def wait_sent(ref, sem):
        pltpu.make_async_remote_copy(
            ref, ref, sem, sem, device_id={"gy": gy}, device_id_type=MESH
        ).wait_send()

    def clear(edge, refs, corners):
        @pl.when(edge)
        def _():
            for ref, way in refs:
                for sweep in range(ITERS):
                    for comp in range(comps):
                        at = ref.at[sweep, comp, way]
                        at[...] = jnp.zeros_like(at)
            for corner in corners:
                for sweep in range(ITERS):
                    for comp in range(comps):
                        at = corner_recv.at[sweep, comp, corner]
                        at[...] = jnp.zeros_like(at)

    clear(gx == 0, ((row_recv, 0), (fine_row_recv, 0)), (0, 2))
    clear(gx == n_gx - 1, ((row_recv, 1), (fine_row_recv, 1)), (1, 3))
    clear(gy == 0, ((col_recv, 0), (fine_col_recv, 0)), (0, 3))
    clear(gy == n_gy - 1, ((col_recv, 1), (fine_col_recv, 1)), (1, 2))

    pl.semaphore_wait(barrier, count - 1)

    def inside(direction):
        dx, dy = DIRECTIONS[direction]
        checks = []
        if dx:
            checks.append(gx > 0 if dx < 0 else gx < n_gx - 1)
        if dy:
            checks.append(gy > 0 if dy < 0 else gy < n_gy - 1)
        return functools.reduce(jnp.logical_and, checks)

    START, MU, KNOWN = 0, comps, comps + 1

    def plane(item, owner, place):
        columns = pl.ds(pl.multiple_of(owner * width, LANES), width)
        lines = pl.ds(pl.multiple_of(place * own_rows, SUB), own_rows)
        if item == MU:
            return coarse_mu.at[:, columns], patch_mu.at[lines, :]
        comp = item - START if item < MU else item - KNOWN
        source, target = (
            (coarse_start, patch_start) if item < MU else (coarse_known, patch_known)
        )
        return source.at[comp, :, columns], target.at[comp, lines, :]

    def each_step(action):
        def body(step, carry):
            action(lax.rem(gy + step, n_gy))
            return carry

        lax.fori_loop(1, n_gy, body, 0)

    def send_moves(item):
        kind = 0 if item < MU else 1 if item == MU else 2

        def send(peer):
            pltpu.make_async_remote_copy(
                *plane(item, peer, gy),
                move_send.at[kind],
                move_recv.at[item],
                device_id={"gy": peer},
                device_id_type=MESH,
            ).start()

        each_step(send)
        pltpu.make_async_copy(*plane(item, gy, gy), move_recv.at[item]).start()

    def wait_moves(item):
        if item == MU:
            target = patch_mu
        elif item < MU:
            target = patch_start.at[item - START]
        else:
            target = patch_known.at[item - KNOWN]
        wait_bytes(target, move_recv.at[item])

    items = 2 * comps + 1

    def open_moves():
        for item in range(1, AHEAD_CENTRAL):
            send_moves(item)

        @pl.when(jnp.logical_not(central))
        def _():
            for item in range(AHEAD_CENTRAL, AHEAD_OUTER):
                send_moves(item)

    def next_moves(item):
        if item + AHEAD_CENTRAL < items:

            @pl.when(central)
            def _():
                send_moves(item + AHEAD_CENTRAL)

        if item + AHEAD_OUTER < items:

            @pl.when(jnp.logical_not(central))
            def _():
                send_moves(item + AHEAD_OUTER)

    half_lane = lane < HALF
    evens_first = jnp.where(half_lane, 2 * lane, 2 * lane - LANES + 1)
    odds_first = jnp.where(half_lane, 2 * lane + 1, 2 * lane - LANES)

    def split_columns(a, b):
        a = jnp.take_along_axis(a, evens_first, axis=1)
        b = jnp.take_along_axis(b, odds_first, axis=1)
        return (
            jnp.where(half_lane, a, b),
            pltpu.roll(jnp.where(half_lane, b, a), HALF, 1),
        )

    def rows_of(block, shift=0):
        if shift == 0:
            return pl.ds(pl.multiple_of(block * SUB + SUB, SUB), SUB)
        return pl.ds(block * SUB + SUB + shift, SUB)

    def plain(block):
        return pl.ds(pl.multiple_of(block * SUB, SUB), SUB)

    inner = pl.ds(SUB, rows)

    def split_field(raw, comp, put):
        def body(block, carry):
            out = []
            for parity in range(2):
                for half in range(halves):
                    at = pl.ds(block * 2 * SUB + parity, SUB, stride=2)
                    both = split_columns(raw[2 * half, comp, at, :], raw[2 * half + 1, comp, at, :])
                    out.append((parity, half, both))
            for parity, half, both in out:
                put(parity, 0, half, block, both[0])
                put(parity, 1, half, block, both[1])
            return carry

        lax.fori_loop(0, blocks, body, 0, unroll=4)

    def split_start(comp):
        def put(parity, side, half, block, cells):
            fine[0][comp, parity, side, half, rows_of(block), :] = cells

        split_field(raw_start, comp, put)

    def split_known(comp):
        def put(parity, side, half, block, cells):
            known[comp, parity, side, half, plain(block), :] = cells

        split_field(raw_known, comp, put)

    def split_mu(block, carry):
        out = []
        for parity in range(2):
            for half in range(halves):
                at = pl.ds(block * 2 * SUB + parity, SUB, stride=2)
                both = split_columns(raw_mu[2 * half, at, :], raw_mu[2 * half + 1, at, :])
                for side in range(2):
                    total = both[side] + 1.0
                    out.append((parity, side, half, total, 1.0 / total))
        for parity, side, half, total, reciprocal in out:
            diag[parity, side, half, plain(block), :] = total
            inverse[parity, side, half, plain(block), :] = reciprocal
        return carry

    def place_mu():
        def body(block, carry):
            total = patch_mu[plain(block), :] + 1.0
            patch_mu[plain(block), :] = total
            patch_inverse[plain(block), :] = 1.0 / total
            return carry

        lax.fori_loop(0, blocks, body, 0, unroll=4)

    def place_start(comp):
        for half in range(halves):
            coarse[0][comp, half, inner, :] = patch_start[
                comp, :, half * LANES : (half + 1) * LANES
            ]

    def message(rows_out, rows_in, cols_out, cols_in, sends, recvs, sweep, comp, direction):
        dx, dy = DIRECTIONS[direction]
        way = direction % 2
        if direction < 2:
            source, target = rows_out.at[sweep, comp, way], rows_in.at[sweep, comp, 1 - way]
        elif direction < 4:
            source, target = cols_out.at[sweep, comp, way], cols_in.at[sweep, comp, 1 - way]
        else:
            source = rows_out.at[sweep, comp, 0 if dx < 0 else 1]
            target = corner_recv.at[sweep, comp, (direction ^ 1) - 4]
        return pltpu.make_async_remote_copy(
            source,
            target,
            sends.at[direction],
            recvs.at[sweep, comp],
            device_id={"gx": gx + dx, "gy": gy + dy},
            device_id_type=MESH,
        )

    fine_message = functools.partial(
        message, fine_row_send, fine_row_recv, fine_col_send, fine_col_recv, fine_send, fine_recv
    )
    coarse_message = functools.partial(
        message, row_send, row_recv, col_send, col_recv, halo_send, halo_recv
    )

    def start_all(of, sweep, comp, directions):
        for direction in directions:

            @pl.when(inside(direction))
            def _():
                of(sweep, comp, direction).start()

    def wait_all(sem, row_units, col_units, corner_units):
        edge_x = jnp.logical_or(gx == 0, gx == n_gx - 1)
        edge_y = jnp.logical_or(gy == 0, gy == n_gy - 1)
        for sides_x, at_x in ((1, edge_x), (2, jnp.logical_not(edge_x))):
            for sides_y, at_y in ((1, edge_y), (2, jnp.logical_not(edge_y))):

                @pl.when(jnp.logical_and(at_x, at_y))
                def _():
                    units = (
                        row_units * sides_x + col_units * sides_y + corner_units * sides_x * sides_y
                    )
                    wait_bytes(tally.at[pl.ds(0, units)], sem)

    all_lanes = lax.broadcasted_iota(jnp.int32, (rows, LANES), 1)
    low = all_lanes < HALF
    middle = jnp.logical_and(all_lanes >= HALF // 2, all_lanes < HALF + HALF // 2)

    def send_fine_cols(sweep, comp):
        buf = sweep % 2
        parts = []
        for parity in range(2):
            if sweep == 0:
                at = pl.ds(parity, rows, stride=2)
                left, right = raw_start[0, comp, at, :], raw_start[tiles - 1, comp, at, :]
            else:
                left = fine[buf][comp, parity, 0, 0, inner, :]
                right = fine[buf][comp, parity, 1, halves - 1, inner, :]
            parts.append(jnp.where(low, left, right))
        turned = jnp.where(middle, pltpu.roll(parts[1], HALF, 1), parts[0]).T
        for way, lines in enumerate(((0, HALF), (LANES - 1, HALF - 1))):
            for parity, line in enumerate(lines):
                fine_col_send[sweep, comp, way, parity : parity + 1, :] = turned[line : line + 1]
        start_all(fine_message, sweep, comp, (2, 3))

    def send_fine_rows(sweep, comp):
        buf = sweep % 2
        for way, line in enumerate((SUB, SUB + rows - 1)):
            for half in range(halves):
                for side in range(2):
                    at = 2 * half + side
                    fine_row_send[sweep, comp, way, at : at + 1, :] = fine[buf][
                        comp, way, side, half, line : line + 1, :
                    ]
        start_all(fine_message, sweep, comp, (0, 1))

    def send_fine(sweep, comp):
        send_fine_cols(sweep, comp)
        send_fine_rows(sweep, comp)

    def take_fine(sweep, comp):
        buf = sweep % 2
        wait_all(fine_recv.at[sweep, comp], tiles, 2 * rows // LANES, 0)
        for half in range(halves):
            for side in range(2):
                at = 2 * half + side
                fine[buf][comp, 1, side, half, SUB - 1 : SUB, :] = fine_row_recv[
                    sweep, comp, 0, at : at + 1, :
                ]
                fine[buf][comp, 0, side, half, SUB + rows : SUB + rows + 1, :] = fine_row_recv[
                    sweep, comp, 1, at : at + 1, :
                ]
        got = [
            [fine_col_recv[sweep, comp, way, p : p + 1, :] for p in range(2)] for way in range(2)
        ]
        fine_halo[comp] = spread_rows(got[0][0], got[1][1], got[0][1], got[1][0])

    def send_coarse(sweep, comp):
        buf = sweep % 2
        for way, line in enumerate((SUB, SUB + rows - 1)):
            for half in range(halves):
                row_send[sweep, comp, way, half : half + 1, :] = coarse[buf][
                    comp, half, line : line + 1, :
                ]
        start_all(coarse_message, sweep, comp, (0, 1, 4, 5, 6, 7))
        turned = jnp.where(
            low, coarse[buf][comp, 0, inner, :], coarse[buf][comp, halves - 1, inner, :]
        ).T
        col_send[sweep, comp, 0] = turned[0:1]
        col_send[sweep, comp, 1] = turned[LANES - 1 : LANES]
        start_all(coarse_message, sweep, comp, (2, 3))

    first_row = lax.broadcasted_iota(jnp.int32, (1, LANES), 1) < HALF

    def take_coarse(sweep, comp):
        buf = sweep % 2
        wait_all(halo_recv.at[sweep, comp], halves, rows // LANES, halves)
        for way, line in enumerate((SUB - 1, SUB + rows)):
            for half in range(halves):
                coarse[buf][comp, half, line : line + 1, :] = row_recv[
                    sweep, comp, way, half : half + 1, :
                ]
        coarse_halo[comp, inner, :] = spread_rows(
            col_recv[sweep, comp, 0], col_recv[sweep, comp, 1]
        )
        for (before, after), line in zip(((0, 2), (3, 1)), (SUB - 1, SUB + rows)):
            left = corner_recv[sweep, comp, before, halves - 1 : halves, :]
            right = corner_recv[sweep, comp, after, 0:1, :]
            coarse_halo[comp, line : line + 1, :] = jnp.where(
                first_row, pltpu.roll(left, 1, 1), pltpu.roll(right, LANES - 1, 1)
            )

    zero = jnp.zeros((SUB, LANES), jnp.float32)

    def coarse_pass(sweep, comp):
        buf = sweep % 2
        last = sweep == ITERS - 1

        def body(block, totals):
            totals = list(totals)
            lines = plain(block)
            out = []
            halo = coarse_halo[comp, rows_of(block), :]
            own = [coarse[buf][comp, half, rows_of(block), :] for half in range(halves)]
            lefts, rights = from_left(own, halo), from_right(own, halo)
            for half in range(halves):
                columns = slice(half * LANES, (half + 1) * LANES)
                near = (
                    coarse[buf][comp, half, rows_of(block, 1), :]
                    + coarse[buf][comp, half, rows_of(block, -1), :]
                    + rights[half]
                    + lefts[half]
                )
                below = (
                    fine[buf][comp, 0, 0, half, rows_of(block), :]
                    + fine[buf][comp, 1, 0, half, rows_of(block), :]
                    + fine[buf][comp, 0, 1, half, rows_of(block), :]
                    + fine[buf][comp, 1, 1, half, rows_of(block), :]
                )
                res = (
                    patch_known[comp, lines, columns]
                    + 0.25 * near
                    + 0.125 * below
                    - patch_mu[lines, columns] * own[half]
                )
                totals[half % 2] = totals[half % 2] + res * res
                out.append((half, own[half] + res * patch_inverse[lines, columns]))
            for half, new in out:
                if last:
                    patch_out[comp, lines, half * LANES : (half + 1) * LANES] = new
                else:
                    coarse[1 - buf][comp, half, rows_of(block), :] = new
            return tuple(totals)

        return sum(lax.fori_loop(0, blocks, body, (zero,) * 2, unroll=4))

    def fine_pass(sweep, comp):
        buf = sweep % 2

        def body(block, totals):
            totals = list(totals)
            out = []
            mid = [coarse[buf][comp, half, rows_of(block), :] for half in range(halves)]
            mid_halo = coarse_halo[comp, rows_of(block), :]
            fine_edges = fine_halo[comp, plain(block), :]
            for parity in range(2):
                shift = 1 if parity else -1
                far_halo = coarse_halo[comp, rows_of(block, shift), :]
                line = [
                    0.75 * mid[half] + 0.25 * coarse[buf][comp, half, rows_of(block, shift), :]
                    for half in range(halves)
                ]
                line_halo = 0.75 * mid_halo + 0.25 * far_halo
                line_left, line_right = from_left(line, line_halo), from_right(line, line_halo)
                edge = roll_lanes(fine_edges, HALF) if parity else fine_edges
                evens, odds = (
                    [fine[buf][comp, parity, side, half, rows_of(block), :] for half in range(halves)]
                    for side in range(2)
                )
                before, after = from_left(odds, edge), from_right(evens, edge)
                for half in range(halves):
                    for side in range(2):
                        own = odds[half] if side else evens[half]
                        lateral = evens[half] + after[half] if side else odds[half] + before[half]
                        near = (
                            fine[buf][comp, 1 - parity, side, half, rows_of(block), :]
                            + fine[buf][comp, 1 - parity, side, half, rows_of(block, shift), :]
                            + lateral
                        )
                        spread = 0.75 * line[half] + 0.25 * (
                            line_right[half] if side else line_left[half]
                        )
                        res = (
                            known[comp, parity, side, half, plain(block), :]
                            + 0.25 * near
                            + 0.5 * spread
                            - diag[parity, side, half, plain(block), :] * own
                        )
                        at = 2 * parity + side
                        totals[at] = totals[at] + res * res
                        new = own + res * inverse[parity, side, half, plain(block), :]
                        out.append((parity, side, half, new))
            for parity, side, half, new in out:
                fine[1 - buf][comp, parity, side, half, rows_of(block), :] = new
            return tuple(totals)

        return sum(lax.fori_loop(0, blocks, body, (zero,) * 4, unroll=2))

    def back_rows(owner):
        return pl.ds(pl.multiple_of(owner * own_rows, SUB), own_rows)

    def back_columns(place):
        return pl.ds(pl.multiple_of(place * width, LANES), width)

    def send_back(comp):
        def send(peer):
            pltpu.make_async_remote_copy(
                patch_out.at[comp, back_rows(peer), :],
                coarse_out.at[comp, :, back_columns(gy)],
                back_send.at[0],
                back_recv.at[0],
                device_id={"gy": peer},
                device_id_type=MESH,
            ).start()

        each_step(send)
        coarse_out[comp, :, back_columns(gy)] = patch_out[comp, back_rows(gy), :]

    weave_a = jnp.where(lane % 2 == 0, lane // 2, lane // 2 + HALF)
    weave_b = jnp.where(lane % 2 == 0, lane // 2 + HALF, lane // 2)
    final = ITERS % 2

    def weave(comp):
        def body(block, carry):
            out = []
            for parity in range(2):
                for half in range(halves):
                    even = fine[final][comp, parity, 0, half, rows_of(block), :]
                    odd = fine[final][comp, parity, 1, half, rows_of(block), :]
                    odd = pltpu.roll(odd, HALF, 1)
                    at = pl.ds(block * 2 * SUB + parity, SUB, stride=2)
                    a = jnp.take_along_axis(jnp.where(half_lane, even, odd), weave_a, axis=1)
                    b = jnp.take_along_axis(jnp.where(half_lane, odd, even), weave_b, axis=1)
                    out.append((2 * half, at, a))
                    out.append((2 * half + 1, at, b))
            for tile, at, cells in out:
                fine_out[tile, comp, at, :] = cells
            return carry

        lax.fori_loop(0, blocks, body, 0, unroll=4)

    totals = [zero] * ITERS

    def on_coarse(sweep, comp):
        totals[sweep] = totals[sweep] + coarse_pass(sweep, comp)

    def on_fine(sweep, comp):
        totals[sweep] = totals[sweep] + fine_pass(sweep, comp)

    def place(comp):
        wait_moves(START + comp)
        place_start(comp)
        send_coarse(0, comp)

    def first_fine(comp):
        take_fine(0, comp)
        take_coarse(0, comp)
        on_fine(0, comp)
        send_fine(1, comp)

    send_moves(START)
    wait_bytes(raw_start, load_sem.at[0])
    for comp in range(comps):
        send_fine_cols(0, comp)
    open_moves()
    for comp in range(comps):
        split_start(comp)
        send_fine_rows(0, comp)
    wait_bytes(raw_mu, load_sem.at[1])
    lax.fori_loop(0, blocks, split_mu, 0, unroll=2)
    wait_bytes(raw_known, load_sem.at[2])
    place(0)
    next_moves(0)
    split_known(0)
    place(1)
    next_moves(1)
    first_fine(0)
    split_known(1)
    place(2)
    next_moves(2)
    first_fine(1)
    split_known(2)
    first_fine(2)
    wait_moves(MU)
    next_moves(MU)
    place_mu()

    def first_coarse(comp):
        wait_moves(KNOWN + comp)
        on_coarse(0, comp)
        send_coarse(1, comp)
        next_moves(KNOWN + comp)

    def second_coarse(comp):
        take_coarse(1, comp)
        on_coarse(1, comp)
        send_coarse(2, comp)

    def second_fine(comp):
        take_fine(1, comp)
        on_fine(1, comp)
        send_fine(2, comp)

    def last_coarse(comp):
        take_coarse(2, comp)
        on_coarse(2, comp)
        send_back(comp)

    def last_fine(comp):
        take_fine(2, comp)
        on_fine(2, comp)

    one_lane = lax.broadcasted_iota(jnp.int32, (1, LANES), 1)

    def gather_sum(sums, sweep):
        return jnp.where(one_lane == sweep, jnp.sum(totals[sweep]), sums)

    first_coarse(0)
    first_coarse(1)
    second_coarse(0)
    second_fine(0)
    first_coarse(2)
    second_coarse(1)
    last_coarse(0)
    second_fine(1)
    second_coarse(2)
    last_coarse(1)
    second_fine(2)
    last_fine(0)
    last_coarse(2)
    sums = jnp.zeros((1, LANES), jnp.float32)
    for sweep in range(ITERS - 1):
        sums = gather_sum(sums, sweep)
    last_fine(1)
    last_fine(2)
    norm_all[me] = gather_sum(sums, ITERS - 1)
    each_device(
        lambda peer: pltpu.make_async_remote_copy(
            norm_all.at[me],
            norm_all.at[me],
            norm_send.at[0],
            norm_recv.at[0],
            device_id=peer,
            device_id_type=MESH,
        ).start()
    )
    for comp in range(comps):
        weave(comp)

    for direction in range(8):
        way = direction % 2 if direction < 4 else 0 if DIRECTIONS[direction][0] < 0 else 1

        @pl.when(inside(direction))
        def _():
            sent = (col_send if direction in (2, 3) else row_send).at[:, :, way]
            wait_sent(sent, halo_send.at[direction])
            if direction < 4:
                sent = (fine_col_send if direction > 1 else fine_row_send).at[:, :, way]
                wait_sent(sent, fine_send.at[direction])

    others = pl.ds(0, rows - own_rows)
    wait_sent(patch_start.at[:, others, :], move_send.at[0])
    wait_sent(patch_mu.at[others, :], move_send.at[1])
    wait_sent(patch_known.at[:, others, :], move_send.at[2])
    wait_sent(patch_out.at[:, others, :], back_send.at[0])
    rest = norm_all.at[pl.ds(0, count - 1)]
    wait_sent(rest, norm_send.at[0])
    wait_bytes(rest, norm_recv.at[0])
    whole = lax.fori_loop(
        0, count, lambda i, acc: acc + norm_all[i], jnp.zeros((1, LANES), jnp.float32)
    )
    norms_out[...] = jnp.broadcast_to(jnp.sqrt(whole / cells_total), norms_out.shape)
    wait_bytes(coarse_out.at[:, :, pl.ds(0, (n_gy - 1) * width)], back_recv.at[0])


def finish(fine_in, coarse_in, norms_in, fine_out, coarse_out, norms_out, sems):
    tiles = fine_in.shape[0]
    copies = [pltpu.make_async_copy(coarse_in, coarse_out, sems.at[tiles])]
    for tile in range(tiles):
        copies.append(
            pltpu.make_async_copy(
                fine_in.at[tile], fine_out.at[:, :, pl.ds(tile * LANES, LANES)], sems.at[tile]
            )
        )
    for copy in copies:
        copy.start()
    for sweep in range(ITERS):
        norms_out[sweep] = norms_in[0, sweep]
    for copy in copies:
        copy.wait()


def on_device(n_gx, n_gy, fine_start, fine_known, fine_mu, coarse_start, coarse_known, coarse_mu):
    comps, fine_rows, fine_cols = fine_start.shape
    rows, width = fine_rows // 2, fine_cols // 2
    halves = width // LANES
    tiles = 2 * halves
    padded = rows + 2 * SUB
    cells_total = 3.0 * (fine_mu.size + coarse_mu.size) * n_gx * n_gy
    f32 = jnp.float32
    dma = pltpu.SemaphoreType.DMA
    anywhere = pl.BlockSpec(memory_space=pl.ANY)
    in_vmem = pl.BlockSpec(memory_space=pltpu.VMEM)
    out_bytes = 4 * (fine_start.size + coarse_start.size + SUB * LANES)
    results = pl.pallas_call(
        functools.partial(kernel, n_gx, n_gy, cells_total),
        out_shape=(
            pltpu.VMEM((tiles, comps, fine_rows, LANES), f32),
            pltpu.VMEM(coarse_start.shape, f32),
            pltpu.VMEM((SUB, LANES), f32),
        ),
        in_specs=[pl.BlockSpec(memory_space=pltpu.HBM)] * 6,
        out_specs=(in_vmem,) * 3,
        scratch_shapes=[
            pltpu.VMEM((tiles, comps, fine_rows, LANES), f32),
            pltpu.VMEM((tiles, comps, fine_rows, LANES), f32),
            pltpu.VMEM((tiles, fine_rows, LANES), f32),
            pltpu.VMEM((comps, 2, 2, halves, padded, LANES), f32),
            pltpu.VMEM((comps, 2, 2, halves, padded, LANES), f32),
            pltpu.VMEM((comps, 2, 2, halves, rows, LANES), f32),
            pltpu.VMEM((2, 2, halves, rows, LANES), f32),
            pltpu.VMEM((2, 2, halves, rows, LANES), f32),
            pltpu.VMEM((comps, rows, width), f32),
            pltpu.VMEM((comps, rows, width), f32),
            pltpu.VMEM((rows, width), f32),
            pltpu.VMEM((rows, width), f32),
            pltpu.VMEM((comps, halves, padded, LANES), f32),
            pltpu.VMEM((comps, halves, padded, LANES), f32),
            pltpu.VMEM((comps, rows, width), f32),
            pltpu.VMEM((ITERS, comps, 2, tiles, LANES), f32),
            pltpu.VMEM((ITERS, comps, 2, tiles, LANES), f32),
            pltpu.VMEM((ITERS, comps, 2, 2, rows), f32),
            pltpu.VMEM((ITERS, comps, 2, 2, rows), f32),
            pltpu.VMEM((ITERS, comps, 2, halves, LANES), f32),
            pltpu.VMEM((ITERS, comps, 2, halves, LANES), f32),
            pltpu.VMEM((ITERS, comps, 2, 1, rows), f32),
            pltpu.VMEM((ITERS, comps, 2, 1, rows), f32),
            pltpu.VMEM((ITERS, comps, 4, halves, LANES), f32),
            pltpu.VMEM((comps, rows, LANES), f32),
            pltpu.VMEM((comps, padded, LANES), f32),
            pltpu.VMEM((n_gx * n_gy, 1, LANES), f32),
            pltpu.VMEM((6 * halves + 4 * rows // LANES, 1, LANES), f32),
            dma((3,)),
            dma((3,)),
            dma((2 * comps + 1,)),
            dma((4,)),
            dma((ITERS, comps)),
            dma((8,)),
            dma((ITERS, comps)),
            dma((1,)),
            dma((1,)),
            dma((1,)),
            dma((1,)),
        ],
        compiler_params=pltpu.CompilerParams(
            collective_id=0,
            has_side_effects=True,
            vmem_limit_bytes=VMEM_BYTES - out_bytes - 2 * SUB * LANES * 4,
        ),
    )(fine_start, fine_known, fine_mu, coarse_start, coarse_known, coarse_mu)
    return pl.pallas_call(
        finish,
        out_shape=(
            jax.ShapeDtypeStruct(fine_start.shape, f32),
            jax.ShapeDtypeStruct(coarse_start.shape, f32),
            jax.ShapeDtypeStruct((ITERS,), f32),
        ),
        in_specs=[in_vmem] * 3,
        out_specs=(anywhere, anywhere, pl.BlockSpec(memory_space=pltpu.SMEM)),
        scratch_shapes=[dma((tiles + 1,))],
        compiler_params=pltpu.CompilerParams(vmem_limit_bytes=2**20),
    )(*(pltpu.with_memory_space_constraint(result, pltpu.VMEM) for result in results))


def solution(mesh):
    n_gx, n_gy = mesh.shape["gx"], mesh.shape["gy"]
    return jax.shard_map(
        functools.partial(on_device, n_gx, n_gy),
        mesh=mesh,
        in_specs=(
            P(None, "gx", "gy"),
            P(None, "gx", "gy"),
            P("gx", "gy"),
            P(None, ("gx", "gy"), None),
            P(None, ("gx", "gy"), None),
            P(("gx", "gy"), None),
        ),
        out_specs=(P(None, "gx", "gy"), P(None, ("gx", "gy"), None), P()),
        check_vma=False,
    )
```

```python
import functools

import jax
import jax.numpy as jnp
from jax import lax
from jax.experimental import pallas as pl
from jax.experimental.pallas import tpu as pltpu
from jax.sharding import PartitionSpec as P

ITERS = 3
LANES = 128
SUB = 8
HALF = LANES // 2
VMEM_BYTES = 67043328
MESH = pl.DeviceIdType.MESH
DIRECTIONS = ((-1, 0), (1, 0), (0, -1), (0, 1))
QUARTER = LANES // 4
REACH = 4
FINE_UNROLL = 8
COARSE_UNROLL = 16
SPLIT_UNROLL = 8
MU_UNROLL = 8


def lane_index():
    return lax.broadcasted_iota(jnp.int32, (SUB, LANES), 1)


def roll_lanes(cells, shift):
    shift = shift % LANES
    return cells if shift == 0 else pltpu.roll(cells, shift, 1)


def beside_left(halves, halo):
    first = lane_index() == 0
    rolled = [roll_lanes(cells, 1) for cells in halves]
    return [jnp.where(first, before, own) for before, own in zip([halo] + rolled[:-1], rolled)]


def beside_right(halves, halo):
    last = lane_index() == LANES - 1
    rolled = [roll_lanes(cells, LANES - 1) for cells in halves]
    return [jnp.where(last, after, own) for own, after in zip(rolled, rolled[1:] + [halo])]


def from_left(ring):
    first = lane_index() == 0
    rolled = [roll_lanes(cells, 1) for cells in ring]
    return [jnp.where(first, rolled[at - 1], rolled[at]) for at in range(len(ring))]


def from_right(ring):
    last = lane_index() == LANES - 1
    rolled = [roll_lanes(cells, LANES - 1) for cells in ring]
    return [jnp.where(last, rolled[at + 1 - len(ring)], rolled[at]) for at in range(len(ring))]


def kernel(
    n_gx,
    n_gy,
    cells_total,
    fine_start,
    fine_known,
    fine_mu,
    coarse_start,
    coarse_known,
    coarse_mu,
    fine_out,
    coarse_out,
    norms_out,
    raw_start,
    raw_known,
    raw_mu,
    fine_a,
    fine_b,
    known,
    diag,
    inverse,
    patch_start,
    patch_known,
    patch_mu,
    patch_inverse,
    coarse_a,
    coarse_b,
    patch_out,
    fine_row_send,
    fine_row_recv,
    fine_col_send,
    fine_col_recv,
    row_send,
    row_recv,
    fine_halo,
    own_planes,
    strip_send,
    strip_recv,
    strip_known,
    strip_mu,
    strip_inverse,
    norm_all,
    tally,
    load_sem,
    move_send,
    move_recv,
    fine_send,
    fine_recv,
    halo_send,
    halo_recv,
    back_send,
    back_recv,
    norm_send,
    norm_recv,
    edge_send,
    edge_recv,
):
    gx = lax.axis_index("gx")
    gy = lax.axis_index("gy")
    me = gx * n_gy + gy
    count = n_gx * n_gy
    fine, coarse = (fine_a, fine_b), (coarse_a, coarse_b)
    comps, rows, width = patch_start.shape
    halves = width // LANES
    tiles = 2 * halves
    blocks = rows // SUB
    own_rows = coarse_start.shape[1]
    lane = lane_index()
    barrier = pltpu.get_barrier_semaphore()

    def each_device(action):
        def along_gx(dx, carry):
            def along_gy(dy, inner_carry):
                action({"gx": lax.rem(gx + dx, n_gx), "gy": lax.rem(gy + dy, n_gy)})
                return inner_carry

            return lax.fori_loop(jnp.where(dx == 0, 1, 0), n_gy, along_gy, carry)

        lax.fori_loop(0, n_gx, along_gx, 0)

    each_device(
        lambda peer: pl.semaphore_signal(barrier, inc=1, device_id=peer, device_id_type=MESH)
    )

    loads = []
    for which, (source, target) in enumerate(
        ((fine_start, raw_start), (fine_mu, raw_mu), (fine_known, raw_known))
    ):
        for tile in range(tiles):
            at = pl.ds(tile * LANES, LANES)
            view = source.at[:, at] if len(source.shape) == 2 else source.at[:, :, at]
            loads.append(
                pltpu.make_async_copy(view, target.at[tile], load_sem.at[which])
            )
    for copy in loads:
        copy.start()

    def wait_bytes(ref, sem):
        pltpu.make_async_copy(ref, ref, sem).wait()

    def wait_sent(ref, sem):
        pltpu.make_async_remote_copy(
            ref, ref, sem, sem, device_id={"gy": gy}, device_id_type=MESH
        ).wait_send()

    pltpu.make_async_copy(coarse_start, own_planes.at[pl.ds(0, comps)], load_sem.at[3]).start()
    pltpu.make_async_copy(coarse_mu, own_planes.at[comps], load_sem.at[3]).start()
    pltpu.make_async_copy(
        coarse_known, own_planes.at[pl.ds(comps + 1, comps)], load_sem.at[3]
    ).start()

    def clear(edge, ref, way):
        @pl.when(edge)
        def _():
            for sweep in range(ITERS):
                for comp in range(comps):
                    at = ref.at[sweep, comp, way]
                    at[...] = jnp.zeros_like(at)

    for ref in (row_recv, fine_row_recv):
        clear(gx == 0, ref, 0)
        clear(gx == n_gx - 1, ref, 1)
    clear(gy == 0, fine_col_recv, 0)
    clear(gy == n_gy - 1, fine_col_recv, 1)
    row_send[...] = jnp.zeros_like(row_send)

    pl.semaphore_wait(barrier, count - 1)

    def inside(direction):
        dx, dy = DIRECTIONS[direction]
        checks = []
        if dx:
            checks.append(gx > 0 if dx < 0 else gx < n_gx - 1)
        if dy:
            checks.append(gy > 0 if dy < 0 else gy < n_gy - 1)
        return functools.reduce(jnp.logical_and, checks)

    START, MU, KNOWN = 0, comps, comps + 1

    def plane(item, owner, place):
        columns = pl.ds(pl.multiple_of(owner * width, LANES), width)
        lines = pl.ds(pl.multiple_of(place * own_rows, SUB), own_rows)
        if item == MU:
            return coarse_mu.at[:, columns], patch_mu.at[lines, :]
        comp = item - START if item < MU else item - KNOWN
        source, target = (
            (coarse_start, patch_start) if item < MU else (coarse_known, patch_known)
        )
        return source.at[comp, :, columns], target.at[comp, lines, :]

    def each_step(action):
        def body(step, carry):
            action(lax.rem(gy + step, n_gy))
            return carry

        lax.fori_loop(1, n_gy, body, 0)

    def send_moves(item):
        kind = 0 if item < MU else 1 if item == MU else 2

        def send(peer):
            pltpu.make_async_remote_copy(
                *plane(item, peer, gy),
                move_send.at[kind],
                move_recv.at[item],
                device_id={"gy": peer},
                device_id_type=MESH,
            ).start()

        each_step(send)
        pltpu.make_async_copy(*plane(item, gy, gy), move_recv.at[item]).start()

    def wait_moves(item):
        if item == MU:
            target = patch_mu
        elif item < MU:
            target = patch_start.at[item - START]
        else:
            target = patch_known.at[item - KNOWN]
        wait_bytes(target, move_recv.at[item])

    items = 2 * comps + 1
    half_lane = lane < HALF
    valid = jnp.where(half_lane, jnp.where(gy < n_gy - 1, 1, 0), jnp.where(gy > 0, 1, 0)) == 1
    own_tiles = own_rows // SUB
    share = LANES // own_tiles

    def strip_at(tile, item):
        return tile * share + 2 * REACH * item

    def send_strips():
        wait_bytes(own_planes, load_sem.at[3])
        for owner in range(n_gy):
            cells = jnp.zeros((SUB, LANES), jnp.float32)
            for tile in range(own_tiles):
                lines = slice(tile * SUB, (tile + 1) * SUB)
                for item in range(items):
                    sides = []
                    for at in (halves * (owner + 1), halves * owner - 1):
                        at = at if 0 <= at < n_gy * halves else 0
                        sides.append(own_planes[item, lines, at * LANES : (at + 1) * LANES])
                    both = jnp.where(half_lane, *sides)
                    start = strip_at(tile, item)
                    here = jnp.logical_and(lane >= start, lane < start + 2 * REACH)
                    cells = jnp.where(here, roll_lanes(both, start + REACH), cells)
            strip_send[owner] = cells

        def send(peer):
            pltpu.make_async_remote_copy(
                strip_send.at[peer],
                strip_recv.at[gy],
                edge_send.at[0],
                edge_recv.at[0],
                device_id={"gy": peer},
                device_id_type=MESH,
            ).start()

        each_step(send)

    def take_strips():
        strip_recv[gy] = strip_send[gy]
        wait_bytes(strip_recv.at[pl.ds(0, n_gy - 1)], edge_recv.at[0])

        def body(owner, carry):
            cells = strip_recv[owner]
            for tile in range(own_tiles):
                block = owner * own_tiles + tile
                for item in range(items):
                    strip = roll_lanes(cells, -strip_at(tile, item) - REACH)
                    if item < MU:
                        coarse[0][item, halves, rows_of(block), :] = jnp.where(valid, strip, 0.0)
                    elif item == MU:
                        strip_mu[plain(block), :] = strip + 1.0
                        strip_inverse[plain(block), :] = 1.0 / (strip + 1.0)
                    else:
                        strip_known[item - KNOWN, plain(block), :] = strip
            return carry

        lax.fori_loop(0, n_gy, body, 0, unroll=2)

    evens_first = jnp.where(half_lane, 2 * lane, 2 * lane - LANES + 1)
    odds_first = jnp.where(half_lane, 2 * lane + 1, 2 * lane - LANES)

    def split_columns(a, b):
        a = jnp.take_along_axis(a, evens_first, axis=1)
        b = jnp.take_along_axis(b, odds_first, axis=1)
        return (
            jnp.where(half_lane, a, b),
            pltpu.roll(jnp.where(half_lane, b, a), HALF, 1),
        )

    def rows_of(block, shift=0):
        if shift == 0:
            return pl.ds(pl.multiple_of(block * SUB + SUB, SUB), SUB)
        return pl.ds(block * SUB + SUB + shift, SUB)

    def plain(block):
        return pl.ds(pl.multiple_of(block * SUB, SUB), SUB)

    inner = pl.ds(SUB, rows)

    def split_field(raw, comp, put):
        def body(block, carry):
            out = []
            for parity in range(2):
                for half in range(halves):
                    at = pl.ds(block * 2 * SUB + parity, SUB, stride=2)
                    both = split_columns(raw[2 * half, comp, at, :], raw[2 * half + 1, comp, at, :])
                    out.append((parity, half, both))
            for parity, half, both in out:
                put(parity, 0, half, block, both[0])
                put(parity, 1, half, block, both[1])
            return carry

        lax.fori_loop(0, blocks, body, 0, unroll=SPLIT_UNROLL)

    def split_start(comp):
        def put(parity, side, half, block, cells):
            fine[0][comp, parity, side, half, rows_of(block), :] = cells

        split_field(raw_start, comp, put)

    def split_known(comp):
        def put(parity, side, half, block, cells):
            known[comp, parity, side, half, plain(block), :] = cells

        split_field(raw_known, comp, put)

    def split_mu(block, carry):
        out = []
        for parity in range(2):
            for half in range(halves):
                at = pl.ds(block * 2 * SUB + parity, SUB, stride=2)
                both = split_columns(raw_mu[2 * half, at, :], raw_mu[2 * half + 1, at, :])
                for side in range(2):
                    total = both[side] + 1.0
                    out.append((parity, side, half, total, 1.0 / total))
        for parity, side, half, total, reciprocal in out:
            diag[parity, side, half, plain(block), :] = total
            inverse[parity, side, half, plain(block), :] = reciprocal
        return carry

    def place_mu():
        def body(block, carry):
            total = patch_mu[plain(block), :] + 1.0
            patch_mu[plain(block), :] = total
            patch_inverse[plain(block), :] = 1.0 / total
            return carry

        lax.fori_loop(0, blocks, body, 0, unroll=4)

    def place_start(comp):
        for half in range(halves):
            coarse[0][comp, half, inner, :] = patch_start[
                comp, :, half * LANES : (half + 1) * LANES
            ]

    def message(direction, source, target, send, recv):
        dx, dy = DIRECTIONS[direction]

        @pl.when(inside(direction))
        def _():
            pltpu.make_async_remote_copy(
                source,
                target,
                send.at[direction],
                recv,
                device_id={"gx": gx + dx, "gy": gy + dy},
                device_id_type=MESH,
            ).start()

    edge_x = jnp.logical_or(gx == 0, gx == n_gx - 1)
    edge_y = jnp.logical_or(gy == 0, gy == n_gy - 1)
    sides_x = ((1, edge_x), (2, jnp.logical_not(edge_x)))
    sides_y = ((1, edge_y), (2, jnp.logical_not(edge_y)))

    all_lanes = lax.broadcasted_iota(jnp.int32, (rows, LANES), 1)
    low = all_lanes < HALF
    middle = jnp.logical_and(all_lanes >= HALF, all_lanes < HALF + QUARTER)
    middle = jnp.logical_or(middle, jnp.logical_and(all_lanes >= HALF - SUB, all_lanes < HALF))
    beside = jnp.logical_and(all_lanes >= QUARTER - REACH, all_lanes < QUARTER + REACH)

    def send_fine_cols(sweep, comp):
        buf = sweep % 2
        parts, sums = [], []
        for parity in range(2):
            if sweep == 0:
                at = pl.ds(parity, rows, stride=2)
                ends = [raw_start[0, comp, at, :], raw_start[tiles - 1, comp, at, :]]
                sums.append(ends)
            else:
                ends = [
                    fine[buf][comp, parity, side, half, inner, :]
                    for side, half in ((0, 0), (1, halves - 1))
                ]
                others = [
                    fine[buf][comp, parity, 1 - side, half, inner, :]
                    for side, half in ((0, 0), (1, halves - 1))
                ]
                sums.append([a + b for a, b in zip(ends, others)])
            parts.append(jnp.where(low, *ends))
        total = jnp.where(low, sums[0][0] + sums[1][0], sums[0][1] + sums[1][1])
        pitch = 1
        if sweep == 0:
            total = total + pltpu.roll(total, LANES - 1, 1)
            pitch = 2
        mixed = jnp.where(middle, pltpu.roll(parts[1], HALF, 1), parts[0])
        turned = jnp.where(beside, pltpu.roll(total, QUARTER, 1), mixed).T
        first = (0, HALF, QUARTER, QUARTER + pitch)
        last = (LANES - 1, HALF - 1, QUARTER - pitch, QUARTER - 2 * pitch)
        for way, lines in enumerate((first, last)):
            for at, line in enumerate(lines):
                fine_col_send[sweep, comp, way, at : at + 1, :] = turned[line : line + 1]
            message(
                2 + way,
                fine_col_send.at[sweep, comp, way],
                fine_col_recv.at[sweep, comp, 1 - way],
                fine_send,
                fine_recv.at[sweep, comp],
            )

    def send_fine_rows(sweep, comp):
        buf = sweep % 2
        for way, line in enumerate((SUB, SUB + rows - 1)):
            for half in range(halves):
                for side in range(2):
                    at = 2 * half + side
                    fine_row_send[sweep, comp, way, at : at + 1, :] = fine[buf][
                        comp, way, side, half, line : line + 1, :
                    ]
            message(
                way,
                fine_row_send.at[sweep, comp, way],
                fine_row_recv.at[sweep, comp, 1 - way],
                fine_send,
                fine_recv.at[sweep, comp],
            )

    def send_fine(sweep, comp):
        send_fine_cols(sweep, comp)
        send_fine_rows(sweep, comp)

    line_at = lax.broadcasted_iota(jnp.int32, (SUB, rows), 0)

    def take_fine(sweep, comp):
        buf = sweep % 2
        for count_x, at_x in sides_x:
            for count_y, at_y in sides_y:

                @pl.when(jnp.logical_and(at_x, at_y))
                def _():
                    units = tiles * count_x + 4 * rows // LANES * count_y
                    wait_bytes(tally.at[pl.ds(0, units)], fine_recv.at[sweep, comp])

        for half in range(halves):
            for side in range(2):
                at = 2 * half + side
                fine[buf][comp, 1, side, half, SUB - 1 : SUB, :] = fine_row_recv[
                    sweep, comp, 0, at : at + 1, :
                ]
                fine[buf][comp, 0, side, half, SUB + rows : SUB + rows + 1, :] = fine_row_recv[
                    sweep, comp, 1, at : at + 1, :
                ]
        left, right = (
            [
                jnp.broadcast_to(fine_col_recv[sweep, comp, way, at : at + 1, :], (SUB, rows))
                for at in range(4)
            ]
            for way in range(2)
        )
        near_left = jnp.where(line_at == SUB - 1, left[2], left[3])
        near_right = jnp.where(line_at == 0, right[2], right[3])
        turned = jnp.concatenate(
            [left[0]] * 3
            + [near_left, near_right]
            + [right[1]] * 3
            + [left[1]] * 4
            + [right[0]] * 4,
            axis=0,
        )
        fine_halo[comp] = turned.T

    def send_coarse(sweep, comp):
        buf = sweep % 2
        for way, line in enumerate((SUB, SUB + rows - 1)):
            for tile in range(halves + 1):
                row_send[sweep, comp, way, tile : tile + 1, :] = coarse[buf][
                    comp, tile, line : line + 1, :
                ]
            message(
                way,
                row_send.at[sweep, comp, way],
                row_recv.at[sweep, comp, 1 - way],
                halo_send,
                halo_recv.at[sweep, comp],
            )

    def take_coarse(sweep, comp):
        buf = sweep % 2
        for count_x, at_x in sides_x:

            @pl.when(at_x)
            def _():
                units = row_send.shape[3] * count_x
                wait_bytes(tally.at[pl.ds(0, units)], halo_recv.at[sweep, comp])

        for way, line in enumerate((SUB - 1, SUB + rows)):
            for tile in range(halves + 1):
                coarse[buf][comp, tile, line : line + 1, :] = row_recv[
                    sweep, comp, way, tile : tile + 1, :
                ]

    zero = jnp.zeros((SUB, LANES), jnp.float32)

    def coarse_pass(sweep, comp):
        buf = sweep % 2
        last = sweep == ITERS - 1

        def body(block, totals):
            totals = list(totals)
            lines = plain(block)
            out = []
            ring = [coarse[buf][comp, tile, rows_of(block), :] for tile in range(halves + 1)]
            lefts, rights = from_left(ring), from_right(ring)
            for tile in range(halves if last else halves + 1):
                columns = slice(tile * LANES, (tile + 1) * LANES)
                near = (
                    coarse[buf][comp, tile, rows_of(block, 1), :]
                    + coarse[buf][comp, tile, rows_of(block, -1), :]
                    + rights[tile]
                    + lefts[tile]
                )
                if tile < halves:
                    below = (
                        fine[buf][comp, 0, 0, tile, rows_of(block), :]
                        + fine[buf][comp, 1, 0, tile, rows_of(block), :]
                        + fine[buf][comp, 0, 1, tile, rows_of(block), :]
                        + fine[buf][comp, 1, 1, tile, rows_of(block), :]
                    )
                    given = patch_known[comp, lines, columns]
                    scale, reciprocal = patch_mu[lines, columns], patch_inverse[lines, columns]
                else:
                    below = roll_lanes(fine_halo[comp, lines, :], -QUARTER)
                    given = strip_known[comp, lines, :]
                    scale, reciprocal = strip_mu[lines, :], strip_inverse[lines, :]
                res = given + 0.25 * near + 0.125 * below - scale * ring[tile]
                new = ring[tile] + res * reciprocal
                if tile < halves:
                    totals[tile % 2] = totals[tile % 2] + res * res
                else:
                    new = jnp.where(valid, new, 0.0)
                out.append((tile, new))
            for tile, new in out:
                if last:
                    patch_out[comp, lines, tile * LANES : (tile + 1) * LANES] = new
                else:
                    coarse[1 - buf][comp, tile, rows_of(block), :] = new
            return tuple(totals)

        return sum(lax.fori_loop(0, blocks, body, (zero,) * 2, unroll=COARSE_UNROLL))

    def fine_pass(sweep, comp):
        buf = sweep % 2

        def body(block, totals):
            totals = list(totals)
            out = []
            mid = [coarse[buf][comp, tile, rows_of(block), :] for tile in range(halves + 1)]
            fine_edges = fine_halo[comp, plain(block), :]
            for parity in range(2):
                shift = 1 if parity else -1
                line = [
                    0.75 * mid[tile] + 0.25 * coarse[buf][comp, tile, rows_of(block, shift), :]
                    for tile in range(halves + 1)
                ]
                line_left, line_right = from_left(line), from_right(line)
                edge = roll_lanes(fine_edges, HALF) if parity else fine_edges
                evens, odds = (
                    [fine[buf][comp, parity, side, half, rows_of(block), :] for half in range(halves)]
                    for side in range(2)
                )
                before, after = beside_left(odds, edge), beside_right(evens, edge)
                for half in range(halves):
                    for side in range(2):
                        own = odds[half] if side else evens[half]
                        lateral = evens[half] + after[half] if side else odds[half] + before[half]
                        near = (
                            fine[buf][comp, 1 - parity, side, half, rows_of(block), :]
                            + fine[buf][comp, 1 - parity, side, half, rows_of(block, shift), :]
                            + lateral
                        )
                        spread = 0.75 * line[half] + 0.25 * (
                            line_right[half] if side else line_left[half]
                        )
                        res = (
                            known[comp, parity, side, half, plain(block), :]
                            + 0.25 * near
                            + 0.5 * spread
                            - diag[parity, side, half, plain(block), :] * own
                        )
                        at = 2 * parity + side
                        totals[at] = totals[at] + res * res
                        new = own + res * inverse[parity, side, half, plain(block), :]
                        out.append((parity, side, half, new))
            for parity, side, half, new in out:
                fine[1 - buf][comp, parity, side, half, rows_of(block), :] = new
            return tuple(totals)

        return sum(lax.fori_loop(0, blocks, body, (zero,) * 4, unroll=FINE_UNROLL))

    def back_rows(owner):
        return pl.ds(pl.multiple_of(owner * own_rows, SUB), own_rows)

    def back_columns(place):
        return pl.ds(pl.multiple_of(place * width, LANES), width)

    def send_back(comp):
        def send(peer):
            pltpu.make_async_remote_copy(
                patch_out.at[comp, back_rows(peer), :],
                coarse_out.at[comp, :, back_columns(gy)],
                back_send.at[0],
                back_recv.at[0],
                device_id={"gy": peer},
                device_id_type=MESH,
            ).start()

        each_step(send)
        coarse_out[comp, :, back_columns(gy)] = patch_out[comp, back_rows(gy), :]

    weave_a = jnp.where(lane % 2 == 0, lane // 2, lane // 2 + HALF)
    weave_b = jnp.where(lane % 2 == 0, lane // 2 + HALF, lane // 2)
    final = ITERS % 2

    def weave(comp):
        def body(block, carry):
            out = []
            for parity in range(2):
                for half in range(halves):
                    even = fine[final][comp, parity, 0, half, rows_of(block), :]
                    odd = fine[final][comp, parity, 1, half, rows_of(block), :]
                    odd = pltpu.roll(odd, HALF, 1)
                    at = pl.ds(block * 2 * SUB + parity, SUB, stride=2)
                    a = jnp.take_along_axis(jnp.where(half_lane, even, odd), weave_a, axis=1)
                    b = jnp.take_along_axis(jnp.where(half_lane, odd, even), weave_b, axis=1)
                    out.append((2 * half, at, a))
                    out.append((2 * half + 1, at, b))
            for tile, at, cells in out:
                fine_out[tile, comp, at, :] = cells
            return carry

        lax.fori_loop(0, blocks, body, 0, unroll=SPLIT_UNROLL)

    totals = [zero] * ITERS

    def on_coarse(sweep, comp):
        totals[sweep] = totals[sweep] + coarse_pass(sweep, comp)

    def on_fine(sweep, comp):
        totals[sweep] = totals[sweep] + fine_pass(sweep, comp)

    def place(comp):
        wait_moves(START + comp)
        place_start(comp)
        send_coarse(0, comp)

    def first_fine(comp):
        take_fine(0, comp)
        take_coarse(0, comp)
        on_fine(0, comp)
        send_fine(1, comp)

    def first_coarse(comp):
        wait_moves(KNOWN + comp)
        on_coarse(0, comp)
        send_coarse(1, comp)

    def second_coarse(comp):
        take_fine(1, comp)
        take_coarse(1, comp)
        on_coarse(1, comp)
        send_coarse(2, comp)

    def second_fine(comp):
        on_fine(1, comp)
        send_fine(2, comp)

    def last_coarse(comp):
        take_coarse(2, comp)
        on_coarse(2, comp)
        send_back(comp)

    def last_fine(comp):
        take_fine(2, comp)
        on_fine(2, comp)

    one_lane = lax.broadcasted_iota(jnp.int32, (1, LANES), 1)

    def gather_sum(sums, sweep):
        return jnp.where(one_lane == sweep, jnp.sum(totals[sweep]), sums)

    send_moves(START)
    send_strips()
    wait_bytes(raw_start, load_sem.at[0])
    for comp in range(comps):
        send_fine_cols(0, comp)
    send_moves(START + 1)
    send_moves(START + 2)
    send_moves(MU)
    send_moves(KNOWN)
    send_moves(KNOWN + 1)
    send_moves(KNOWN + 2)
    split_start(0)
    send_fine_rows(0, 0)
    split_start(1)
    send_fine_rows(0, 1)
    split_start(2)
    send_fine_rows(0, 2)
    wait_bytes(raw_mu, load_sem.at[1])
    lax.fori_loop(0, blocks, split_mu, 0, unroll=MU_UNROLL)
    wait_bytes(raw_known, load_sem.at[2])
    split_known(0)
    split_known(1)
    split_known(2)
    take_strips()
    place(0)
    first_fine(0)
    place(1)
    first_fine(1)
    place(2)
    first_fine(2)
    wait_moves(MU)
    place_mu()
    first_coarse(0)
    first_coarse(1)
    first_coarse(2)
    second_coarse(0)
    second_fine(0)
    second_coarse(1)
    second_fine(1)
    last_coarse(0)
    second_coarse(2)
    second_fine(2)
    last_coarse(1)
    last_coarse(2)
    last_fine(0)
    last_fine(1)
    sums = jnp.zeros((1, LANES), jnp.float32)
    for sweep in range(ITERS - 1):
        sums = gather_sum(sums, sweep)
    last_fine(2)
    norm_all[me] = gather_sum(sums, ITERS - 1)
    each_device(
        lambda peer: pltpu.make_async_remote_copy(
            norm_all.at[me],
            norm_all.at[me],
            norm_send.at[0],
            norm_recv.at[0],
            device_id=peer,
            device_id_type=MESH,
        ).start()
    )
    weave(0)
    weave(1)
    weave(2)

    for direction in range(4):
        way = direction % 2

        @pl.when(inside(direction))
        def _():
            sent = (fine_row_send if direction < 2 else fine_col_send).at[:, :, way]
            wait_sent(sent, fine_send.at[direction])
            if direction < 2:
                wait_sent(row_send.at[:, :, way], halo_send.at[direction])

    wait_sent(strip_send.at[pl.ds(0, n_gy - 1)], edge_send.at[0])
    others = pl.ds(0, rows - own_rows)
    wait_sent(patch_start.at[:, others, :], move_send.at[0])
    wait_sent(patch_mu.at[others, :], move_send.at[1])
    wait_sent(patch_known.at[:, others, :], move_send.at[2])
    wait_sent(patch_out.at[:, others, :], back_send.at[0])
    rest = norm_all.at[pl.ds(0, count - 1)]
    wait_sent(rest, norm_send.at[0])
    wait_bytes(rest, norm_recv.at[0])
    whole = lax.fori_loop(
        0, count, lambda i, acc: acc + norm_all[i], jnp.zeros((1, LANES), jnp.float32)
    )
    norms_out[...] = jnp.broadcast_to(jnp.sqrt(whole / cells_total), norms_out.shape)
    wait_bytes(coarse_out.at[:, :, pl.ds(0, (n_gy - 1) * width)], back_recv.at[0])


def finish(fine_in, coarse_in, norms_in, fine_out, coarse_out, norms_out, sems):
    tiles = fine_in.shape[0]
    copies = [pltpu.make_async_copy(coarse_in, coarse_out, sems.at[tiles])]
    for tile in range(tiles):
        copies.append(
            pltpu.make_async_copy(
                fine_in.at[tile], fine_out.at[:, :, pl.ds(tile * LANES, LANES)], sems.at[tile]
            )
        )
    for copy in copies:
        copy.start()
    for sweep in range(ITERS):
        norms_out[sweep] = norms_in[0, sweep]
    for copy in copies:
        copy.wait()


def on_device(n_gx, n_gy, fine_start, fine_known, fine_mu, coarse_start, coarse_known, coarse_mu):
    comps, fine_rows, fine_cols = fine_start.shape
    rows, width = fine_rows // 2, fine_cols // 2
    halves = width // LANES
    tiles = 2 * halves
    padded = rows + 2 * SUB
    row_pad = 1 << halves.bit_length()
    cells_total = 3.0 * (fine_mu.size + coarse_mu.size) * n_gx * n_gy
    f32 = jnp.float32
    dma = pltpu.SemaphoreType.DMA
    anywhere = pl.BlockSpec(memory_space=pl.ANY)
    in_vmem = pl.BlockSpec(memory_space=pltpu.VMEM)
    out_bytes = 4 * (fine_start.size + coarse_start.size + SUB * LANES)
    results = pl.pallas_call(
        functools.partial(kernel, n_gx, n_gy, cells_total),
        out_shape=(
            pltpu.VMEM((tiles, comps, fine_rows, LANES), f32),
            pltpu.VMEM(coarse_start.shape, f32),
            pltpu.VMEM((SUB, LANES), f32),
        ),
        in_specs=[pl.BlockSpec(memory_space=pltpu.HBM)] * 6,
        out_specs=(in_vmem,) * 3,
        scratch_shapes=[
            pltpu.VMEM((tiles, comps, fine_rows, LANES), f32),
            pltpu.VMEM((tiles, comps, fine_rows, LANES), f32),
            pltpu.VMEM((tiles, fine_rows, LANES), f32),
            pltpu.VMEM((comps, 2, 2, halves, padded, LANES), f32),
            pltpu.VMEM((comps, 2, 2, halves, padded, LANES), f32),
            pltpu.VMEM((comps, 2, 2, halves, rows, LANES), f32),
            pltpu.VMEM((2, 2, halves, rows, LANES), f32),
            pltpu.VMEM((2, 2, halves, rows, LANES), f32),
            pltpu.VMEM((comps, rows, width), f32),
            pltpu.VMEM((comps, rows, width), f32),
            pltpu.VMEM((rows, width), f32),
            pltpu.VMEM((rows, width), f32),
            pltpu.VMEM((comps, halves + 1, padded, LANES), f32),
            pltpu.VMEM((comps, halves + 1, padded, LANES), f32),
            pltpu.VMEM((comps, rows, width), f32),
            pltpu.VMEM((ITERS, comps, 2, tiles, LANES), f32),
            pltpu.VMEM((ITERS, comps, 2, tiles, LANES), f32),
            pltpu.VMEM((ITERS, comps, 2, 4, rows), f32),
            pltpu.VMEM((ITERS, comps, 2, 4, rows), f32),
            pltpu.VMEM((ITERS, comps, 2, row_pad, LANES), f32),
            pltpu.VMEM((ITERS, comps, 2, row_pad, LANES), f32),
            pltpu.VMEM((comps, rows, LANES), f32),
            pltpu.VMEM((2 * comps + 1,) + coarse_mu.shape, f32),
            pltpu.VMEM((n_gy, SUB, LANES), f32),
            pltpu.VMEM((n_gy, SUB, LANES), f32),
            pltpu.VMEM((comps, rows, LANES), f32),
            pltpu.VMEM((rows, LANES), f32),
            pltpu.VMEM((rows, LANES), f32),
            pltpu.VMEM((n_gx * n_gy, 1, LANES), f32),
            pltpu.VMEM((2 * tiles + 2 * row_pad + 8 * rows // LANES, 1, LANES), f32),
            dma((4,)),
            dma((3,)),
            dma((2 * comps + 1,)),
            dma((4,)),
            dma((ITERS, comps)),
            dma((2,)),
            dma((ITERS, comps)),
            dma((1,)),
            dma((1,)),
            dma((1,)),
            dma((1,)),
            dma((1,)),
            dma((1,)),
        ],
        compiler_params=pltpu.CompilerParams(
            collective_id=0,
            has_side_effects=True,
            vmem_limit_bytes=VMEM_BYTES - out_bytes - 2 * SUB * LANES * 4,
        ),
    )(fine_start, fine_known, fine_mu, coarse_start, coarse_known, coarse_mu)
    return pl.pallas_call(
        finish,
        out_shape=(
            jax.ShapeDtypeStruct(fine_start.shape, f32),
            jax.ShapeDtypeStruct(coarse_start.shape, f32),
            jax.ShapeDtypeStruct((ITERS,), f32),
        ),
        in_specs=[in_vmem] * 3,
        out_specs=(anywhere, anywhere, pl.BlockSpec(memory_space=pltpu.SMEM)),
        scratch_shapes=[dma((tiles + 1,))],
        compiler_params=pltpu.CompilerParams(vmem_limit_bytes=2**20),
    )(*(pltpu.with_memory_space_constraint(result, pltpu.VMEM) for result in results))


def solution(mesh):
    n_gx, n_gy = mesh.shape["gx"], mesh.shape["gy"]
    return jax.shard_map(
        functools.partial(on_device, n_gx, n_gy),
        mesh=mesh,
        in_specs=(
            P(None, "gx", "gy"),
            P(None, "gx", "gy"),
            P("gx", "gy"),
            P(None, ("gx", "gy"), None),
            P(None, ("gx", "gy"), None),
            P(("gx", "gy"), None),
        ),
        out_specs=(P(None, "gx", "gy"), P(None, ("gx", "gy"), None), P()),
        check_vma=False,
    )
```

```python
import functools

import jax
import jax.numpy as jnp
from jax import lax
from jax.experimental import pallas as pl
from jax.experimental.pallas import tpu as pltpu
from jax.sharding import PartitionSpec as P

ITERS = 3
LANES = 128
SUB = 8
HALF = LANES // 2
VMEM_BYTES = 67043328
MESH = pl.DeviceIdType.MESH
DIRECTIONS = ((-1, 0), (1, 0), (0, -1), (0, 1))
QUARTER = LANES // 4
REACH = 4
FINE_UNROLL = 8
COARSE_UNROLL = 16
SPLIT_UNROLL = 8
MU_UNROLL = 8


def lane_index():
    return lax.broadcasted_iota(jnp.int32, (SUB, LANES), 1)


def roll_lanes(cells, shift):
    shift = shift % LANES
    return cells if shift == 0 else pltpu.roll(cells, shift, 1)


def beside_left(halves, halo):
    first = lane_index() == 0
    rolled = [roll_lanes(cells, 1) for cells in halves]
    return [jnp.where(first, before, own) for before, own in zip([halo] + rolled[:-1], rolled)]


def beside_right(halves, halo):
    last = lane_index() == LANES - 1
    rolled = [roll_lanes(cells, LANES - 1) for cells in halves]
    return [jnp.where(last, after, own) for own, after in zip(rolled, rolled[1:] + [halo])]


def from_left(ring):
    first = lane_index() == 0
    rolled = [roll_lanes(cells, 1) for cells in ring]
    return [jnp.where(first, rolled[at - 1], rolled[at]) for at in range(len(ring))]


def from_right(ring):
    last = lane_index() == LANES - 1
    rolled = [roll_lanes(cells, LANES - 1) for cells in ring]
    return [jnp.where(last, rolled[at + 1 - len(ring)], rolled[at]) for at in range(len(ring))]


def kernel(
    n_gx,
    n_gy,
    cells_total,
    fine_start,
    fine_known,
    fine_mu,
    coarse_start,
    coarse_known,
    coarse_mu,
    fine_out,
    coarse_out,
    norms_out,
    raw_start,
    raw_known,
    raw_mu,
    fine_a,
    fine_b,
    known,
    diag,
    inverse,
    patch_start,
    patch_known,
    patch_mu,
    patch_inverse,
    coarse_a,
    coarse_b,
    patch_out,
    fine_row_send,
    fine_row_recv,
    fine_col_send,
    fine_col_recv,
    row_send,
    row_recv,
    fine_halo,
    own_planes,
    strip_send,
    strip_recv,
    strip_known,
    strip_mu,
    strip_inverse,
    norm_all,
    tally,
    load_sem,
    move_send,
    move_recv,
    fine_send,
    fine_recv,
    halo_send,
    halo_recv,
    back_send,
    back_recv,
    norm_send,
    norm_recv,
    edge_send,
    edge_recv,
):
    gx = lax.axis_index("gx")
    gy = lax.axis_index("gy")
    me = gx * n_gy + gy
    count = n_gx * n_gy
    fine, coarse = (fine_a, fine_b), (coarse_a, coarse_b)
    comps, rows, width = patch_start.shape
    halves = width // LANES
    tiles = 2 * halves
    blocks = rows // SUB
    own_rows = coarse_start.shape[1]
    lane = lane_index()
    barrier = pltpu.get_barrier_semaphore()

    def each_device(action):
        def along_gx(dx, carry):
            def along_gy(dy, inner_carry):
                action({"gx": lax.rem(gx + dx, n_gx), "gy": lax.rem(gy + dy, n_gy)})
                return inner_carry

            return lax.fori_loop(jnp.where(dx == 0, 1, 0), n_gy, along_gy, carry)

        lax.fori_loop(0, n_gx, along_gx, 0)

    each_device(
        lambda peer: pl.semaphore_signal(barrier, inc=1, device_id=peer, device_id_type=MESH)
    )

    pltpu.make_async_copy(coarse_start, own_planes.at[pl.ds(0, comps)], load_sem.at[3]).start()
    pltpu.make_async_copy(coarse_mu, own_planes.at[comps], load_sem.at[3]).start()
    pltpu.make_async_copy(
        coarse_known, own_planes.at[pl.ds(comps + 1, comps)], load_sem.at[3]
    ).start()

    loads = []
    for which, (source, target) in enumerate(
        ((fine_start, raw_start), (fine_mu, raw_mu), (fine_known, raw_known))
    ):
        for tile in range(tiles):
            at = pl.ds(tile * LANES, LANES)
            view = source.at[:, at] if len(source.shape) == 2 else source.at[:, :, at]
            loads.append(
                pltpu.make_async_copy(view, target.at[tile], load_sem.at[which])
            )
    for copy in loads:
        copy.start()

    def wait_bytes(ref, sem):
        pltpu.make_async_copy(ref, ref, sem).wait()

    def wait_sent(ref, sem):
        pltpu.make_async_remote_copy(
            ref, ref, sem, sem, device_id={"gy": gy}, device_id_type=MESH
        ).wait_send()

    def clear(edge, ref, way):
        @pl.when(edge)
        def _():
            for sweep in range(ITERS):
                for comp in range(comps):
                    at = ref.at[sweep, comp, way]
                    at[...] = jnp.zeros_like(at)

    for ref in (row_recv, fine_row_recv):
        clear(gx == 0, ref, 0)
        clear(gx == n_gx - 1, ref, 1)
    clear(gy == 0, fine_col_recv, 0)
    clear(gy == n_gy - 1, fine_col_recv, 1)
    row_send[...] = jnp.zeros_like(row_send)

    pl.semaphore_wait(barrier, count - 1)

    def inside(direction):
        dx, dy = DIRECTIONS[direction]
        checks = []
        if dx:
            checks.append(gx > 0 if dx < 0 else gx < n_gx - 1)
        if dy:
            checks.append(gy > 0 if dy < 0 else gy < n_gy - 1)
        return functools.reduce(jnp.logical_and, checks)

    START, MU, KNOWN = 0, comps, comps + 1

    def plane(item, owner, place):
        columns = pl.ds(pl.multiple_of(owner * width, LANES), width)
        lines = pl.ds(pl.multiple_of(place * own_rows, SUB), own_rows)
        source = own_planes.at[item, :, columns]
        if item == MU:
            return source, patch_mu.at[lines, :]
        if item < MU:
            return source, patch_start.at[item - START, lines, :]
        return source, patch_known.at[item - KNOWN, lines, :]

    def each_step(action):
        def body(step, carry):
            action(lax.rem(gy + step, n_gy))
            return carry

        lax.fori_loop(1, n_gy, body, 0)

    own_columns = pl.ds(pl.multiple_of(gy * width, LANES), width)

    def send_moves(item):
        kind = 0 if item < MU else 1 if item == MU else 2

        def send(peer):
            pltpu.make_async_remote_copy(
                *plane(item, peer, gy),
                move_send.at[kind],
                move_recv.at[item],
                device_id={"gy": peer},
                device_id_type=MESH,
            ).start()

        each_step(send)
        if item == MU:
            source = coarse_mu.at[:, own_columns]
        elif item < MU:
            source = coarse_start.at[item - START, :, own_columns]
        else:
            source = coarse_known.at[item - KNOWN, :, own_columns]
        pltpu.make_async_copy(source, plane(item, gy, gy)[1], move_recv.at[item]).start()

    def wait_moves(item):
        if item == MU:
            target = patch_mu
        elif item < MU:
            target = patch_start.at[item - START]
        else:
            target = patch_known.at[item - KNOWN]
        wait_bytes(target, move_recv.at[item])

    items = 2 * comps + 1
    half_lane = lane < HALF
    valid = jnp.where(half_lane, jnp.where(gy < n_gy - 1, 1, 0), jnp.where(gy > 0, 1, 0)) == 1
    own_tiles = own_rows // SUB
    share = LANES // own_tiles

    def strip_at(tile, item):
        return tile * share + 2 * REACH * item

    def send_strips():
        for owner in range(n_gy):
            cells = jnp.zeros((SUB, LANES), jnp.float32)
            for tile in range(own_tiles):
                lines = slice(tile * SUB, (tile + 1) * SUB)
                for item in range(items):
                    sides = []
                    for at in (halves * (owner + 1), halves * owner - 1):
                        at = at if 0 <= at < n_gy * halves else 0
                        sides.append(own_planes[item, lines, at * LANES : (at + 1) * LANES])
                    both = jnp.where(half_lane, *sides)
                    start = strip_at(tile, item)
                    here = jnp.logical_and(lane >= start, lane < start + 2 * REACH)
                    cells = jnp.where(here, roll_lanes(both, start + REACH), cells)
            strip_send[owner] = cells

        def send(peer):
            pltpu.make_async_remote_copy(
                strip_send.at[peer],
                strip_recv.at[gy],
                edge_send.at[0],
                edge_recv.at[0],
                device_id={"gy": peer},
                device_id_type=MESH,
            ).start()

        each_step(send)

    def take_strips():
        strip_recv[gy] = strip_send[gy]
        wait_bytes(strip_recv.at[pl.ds(0, n_gy - 1)], edge_recv.at[0])

        def body(owner, carry):
            cells = strip_recv[owner]
            for tile in range(own_tiles):
                block = owner * own_tiles + tile
                for item in range(items):
                    strip = roll_lanes(cells, -strip_at(tile, item) - REACH)
                    if item < MU:
                        coarse[0][item, halves, rows_of(block), :] = jnp.where(valid, strip, 0.0)
                    elif item == MU:
                        strip_mu[plain(block), :] = strip + 1.0
                        strip_inverse[plain(block), :] = 1.0 / (strip + 1.0)
                    else:
                        strip_known[item - KNOWN, plain(block), :] = strip
            return carry

        lax.fori_loop(0, n_gy, body, 0, unroll=2)

    evens_first = jnp.where(half_lane, 2 * lane, 2 * lane - LANES + 1)
    odds_first = jnp.where(half_lane, 2 * lane + 1, 2 * lane - LANES)

    def split_columns(a, b):
        a = jnp.take_along_axis(a, evens_first, axis=1)
        b = jnp.take_along_axis(b, odds_first, axis=1)
        return (
            jnp.where(half_lane, a, b),
            pltpu.roll(jnp.where(half_lane, b, a), HALF, 1),
        )

    def rows_of(block, shift=0):
        if shift == 0:
            return pl.ds(pl.multiple_of(block * SUB + SUB, SUB), SUB)
        return pl.ds(block * SUB + SUB + shift, SUB)

    def plain(block):
        return pl.ds(pl.multiple_of(block * SUB, SUB), SUB)

    inner = pl.ds(SUB, rows)

    def split_field(raw, comp, put):
        def body(block, carry):
            out = []
            for parity in range(2):
                for half in range(halves):
                    at = pl.ds(block * 2 * SUB + parity, SUB, stride=2)
                    both = split_columns(raw[2 * half, comp, at, :], raw[2 * half + 1, comp, at, :])
                    out.append((parity, half, both))
            for parity, half, both in out:
                put(parity, 0, half, block, both[0])
                put(parity, 1, half, block, both[1])
            return carry

        lax.fori_loop(0, blocks, body, 0, unroll=SPLIT_UNROLL)

    def split_start(comp):
        def put(parity, side, half, block, cells):
            fine[0][comp, parity, side, half, rows_of(block), :] = cells

        split_field(raw_start, comp, put)

    def split_known(comp):
        def put(parity, side, half, block, cells):
            known[comp, parity, side, half, plain(block), :] = cells

        split_field(raw_known, comp, put)

    def split_mu(block, carry):
        out = []
        for parity in range(2):
            for half in range(halves):
                at = pl.ds(block * 2 * SUB + parity, SUB, stride=2)
                both = split_columns(raw_mu[2 * half, at, :], raw_mu[2 * half + 1, at, :])
                for side in range(2):
                    total = both[side] + 1.0
                    out.append((parity, side, half, total, 1.0 / total))
        for parity, side, half, total, reciprocal in out:
            diag[parity, side, half, plain(block), :] = total
            inverse[parity, side, half, plain(block), :] = reciprocal
        return carry

    def place_mu():
        def body(block, carry):
            total = patch_mu[plain(block), :] + 1.0
            patch_mu[plain(block), :] = total
            patch_inverse[plain(block), :] = 1.0 / total
            return carry

        lax.fori_loop(0, blocks, body, 0, unroll=4)

    def place_start(comp):
        for half in range(halves):
            coarse[0][comp, half, inner, :] = patch_start[
                comp, :, half * LANES : (half + 1) * LANES
            ]

    def message(direction, source, target, send, recv):
        dx, dy = DIRECTIONS[direction]

        @pl.when(inside(direction))
        def _():
            pltpu.make_async_remote_copy(
                source,
                target,
                send.at[direction],
                recv,
                device_id={"gx": gx + dx, "gy": gy + dy},
                device_id_type=MESH,
            ).start()

    edge_x = jnp.logical_or(gx == 0, gx == n_gx - 1)
    edge_y = jnp.logical_or(gy == 0, gy == n_gy - 1)
    sides_x = ((1, edge_x), (2, jnp.logical_not(edge_x)))
    sides_y = ((1, edge_y), (2, jnp.logical_not(edge_y)))

    all_lanes = lax.broadcasted_iota(jnp.int32, (rows, LANES), 1)
    low = all_lanes < HALF
    middle = jnp.logical_and(all_lanes >= HALF, all_lanes < HALF + QUARTER)
    middle = jnp.logical_or(middle, jnp.logical_and(all_lanes >= HALF - SUB, all_lanes < HALF))
    beside = jnp.logical_and(all_lanes >= QUARTER - REACH, all_lanes < QUARTER + REACH)

    def send_fine_cols(sweep, comp):
        buf = sweep % 2
        parts, sums = [], []
        for parity in range(2):
            if sweep == 0:
                at = pl.ds(parity, rows, stride=2)
                ends = [raw_start[0, comp, at, :], raw_start[tiles - 1, comp, at, :]]
                sums.append(ends)
            else:
                ends = [
                    fine[buf][comp, parity, side, half, inner, :]
                    for side, half in ((0, 0), (1, halves - 1))
                ]
                others = [
                    fine[buf][comp, parity, 1 - side, half, inner, :]
                    for side, half in ((0, 0), (1, halves - 1))
                ]
                sums.append([a + b for a, b in zip(ends, others)])
            parts.append(jnp.where(low, *ends))
        total = jnp.where(low, sums[0][0] + sums[1][0], sums[0][1] + sums[1][1])
        pitch = 1
        if sweep == 0:
            total = total + pltpu.roll(total, LANES - 1, 1)
            pitch = 2
        mixed = jnp.where(middle, pltpu.roll(parts[1], HALF, 1), parts[0])
        turned = jnp.where(beside, pltpu.roll(total, QUARTER, 1), mixed).T
        first = (0, HALF, QUARTER, QUARTER + pitch)
        last = (LANES - 1, HALF - 1, QUARTER - pitch, QUARTER - 2 * pitch)
        for way, lines in enumerate((first, last)):
            for at, line in enumerate(lines):
                fine_col_send[sweep, comp, way, at : at + 1, :] = turned[line : line + 1]
            message(
                2 + way,
                fine_col_send.at[sweep, comp, way],
                fine_col_recv.at[sweep, comp, 1 - way],
                fine_send,
                fine_recv.at[sweep, comp],
            )

    def send_fine_rows(sweep, comp):
        buf = sweep % 2
        for way, line in enumerate((SUB, SUB + rows - 1)):
            for half in range(halves):
                for side in range(2):
                    at = 2 * half + side
                    fine_row_send[sweep, comp, way, at : at + 1, :] = fine[buf][
                        comp, way, side, half, line : line + 1, :
                    ]
            message(
                way,
                fine_row_send.at[sweep, comp, way],
                fine_row_recv.at[sweep, comp, 1 - way],
                fine_send,
                fine_recv.at[sweep, comp],
            )

    def send_fine(sweep, comp):
        send_fine_cols(sweep, comp)
        send_fine_rows(sweep, comp)

    line_at = lax.broadcasted_iota(jnp.int32, (SUB, rows), 0)

    def take_fine(sweep, comp):
        buf = sweep % 2
        for count_x, at_x in sides_x:
            for count_y, at_y in sides_y:

                @pl.when(jnp.logical_and(at_x, at_y))
                def _():
                    units = tiles * count_x + 4 * rows // LANES * count_y
                    wait_bytes(tally.at[pl.ds(0, units)], fine_recv.at[sweep, comp])

        for half in range(halves):
            for side in range(2):
                at = 2 * half + side
                fine[buf][comp, 1, side, half, SUB - 1 : SUB, :] = fine_row_recv[
                    sweep, comp, 0, at : at + 1, :
                ]
                fine[buf][comp, 0, side, half, SUB + rows : SUB + rows + 1, :] = fine_row_recv[
                    sweep, comp, 1, at : at + 1, :
                ]
        left, right = (
            [
                jnp.broadcast_to(fine_col_recv[sweep, comp, way, at : at + 1, :], (SUB, rows))
                for at in range(4)
            ]
            for way in range(2)
        )
        near_left = jnp.where(line_at == SUB - 1, left[2], left[3])
        near_right = jnp.where(line_at == 0, right[2], right[3])
        turned = jnp.concatenate(
            [left[0]] * 3
            + [near_left, near_right]
            + [right[1]] * 3
            + [left[1]] * 4
            + [right[0]] * 4,
            axis=0,
        )
        fine_halo[comp] = turned.T

    def send_coarse(sweep, comp):
        buf = sweep % 2
        for way, line in enumerate((SUB, SUB + rows - 1)):
            for tile in range(halves + 1):
                row_send[sweep, comp, way, tile : tile + 1, :] = coarse[buf][
                    comp, tile, line : line + 1, :
                ]
            message(
                way,
                row_send.at[sweep, comp, way],
                row_recv.at[sweep, comp, 1 - way],
                halo_send,
                halo_recv.at[sweep, comp],
            )

    def take_coarse(sweep, comp):
        buf = sweep % 2
        for count_x, at_x in sides_x:

            @pl.when(at_x)
            def _():
                units = row_send.shape[3] * count_x
                wait_bytes(tally.at[pl.ds(0, units)], halo_recv.at[sweep, comp])

        for way, line in enumerate((SUB - 1, SUB + rows)):
            for tile in range(halves + 1):
                coarse[buf][comp, tile, line : line + 1, :] = row_recv[
                    sweep, comp, way, tile : tile + 1, :
                ]

    zero = jnp.zeros((SUB, LANES), jnp.float32)

    def coarse_pass(sweep, comp):
        buf = sweep % 2
        last = sweep == ITERS - 1

        def body(block, totals):
            totals = list(totals)
            lines = plain(block)
            out = []
            ring = [coarse[buf][comp, tile, rows_of(block), :] for tile in range(halves + 1)]
            lefts, rights = from_left(ring), from_right(ring)
            for tile in range(halves if last else halves + 1):
                columns = slice(tile * LANES, (tile + 1) * LANES)
                near = (
                    coarse[buf][comp, tile, rows_of(block, 1), :]
                    + coarse[buf][comp, tile, rows_of(block, -1), :]
                    + rights[tile]
                    + lefts[tile]
                )
                if tile < halves:
                    below = (
                        fine[buf][comp, 0, 0, tile, rows_of(block), :]
                        + fine[buf][comp, 1, 0, tile, rows_of(block), :]
                        + fine[buf][comp, 0, 1, tile, rows_of(block), :]
                        + fine[buf][comp, 1, 1, tile, rows_of(block), :]
                    )
                    given = patch_known[comp, lines, columns]
                    scale, reciprocal = patch_mu[lines, columns], patch_inverse[lines, columns]
                else:
                    below = roll_lanes(fine_halo[comp, lines, :], -QUARTER)
                    given = strip_known[comp, lines, :]
                    scale, reciprocal = strip_mu[lines, :], strip_inverse[lines, :]
                res = given + 0.25 * near + 0.125 * below - scale * ring[tile]
                new = ring[tile] + res * reciprocal
                if tile < halves:
                    totals[tile % 2] = totals[tile % 2] + res * res
                else:
                    new = jnp.where(valid, new, 0.0)
                out.append((tile, new))
            for tile, new in out:
                if last:
                    patch_out[comp, lines, tile * LANES : (tile + 1) * LANES] = new
                else:
                    coarse[1 - buf][comp, tile, rows_of(block), :] = new
            return tuple(totals)

        return sum(lax.fori_loop(0, blocks, body, (zero,) * 2, unroll=COARSE_UNROLL))

    def fine_pass(sweep, comp):
        buf = sweep % 2

        def body(block, totals):
            totals = list(totals)
            out = []
            mid = [coarse[buf][comp, tile, rows_of(block), :] for tile in range(halves + 1)]
            fine_edges = fine_halo[comp, plain(block), :]
            for parity in range(2):
                shift = 1 if parity else -1
                line = [
                    0.75 * mid[tile] + 0.25 * coarse[buf][comp, tile, rows_of(block, shift), :]
                    for tile in range(halves + 1)
                ]
                line_left, line_right = from_left(line), from_right(line)
                edge = roll_lanes(fine_edges, HALF) if parity else fine_edges
                evens, odds = (
                    [fine[buf][comp, parity, side, half, rows_of(block), :] for half in range(halves)]
                    for side in range(2)
                )
                before, after = beside_left(odds, edge), beside_right(evens, edge)
                for half in range(halves):
                    for side in range(2):
                        own = odds[half] if side else evens[half]
                        lateral = evens[half] + after[half] if side else odds[half] + before[half]
                        near = (
                            fine[buf][comp, 1 - parity, side, half, rows_of(block), :]
                            + fine[buf][comp, 1 - parity, side, half, rows_of(block, shift), :]
                            + lateral
                        )
                        spread = 0.75 * line[half] + 0.25 * (
                            line_right[half] if side else line_left[half]
                        )
                        res = (
                            known[comp, parity, side, half, plain(block), :]
                            + 0.25 * near
                            + 0.5 * spread
                            - diag[parity, side, half, plain(block), :] * own
                        )
                        at = 2 * parity + side
                        totals[at] = totals[at] + res * res
                        new = own + res * inverse[parity, side, half, plain(block), :]
                        out.append((parity, side, half, new))
            for parity, side, half, new in out:
                fine[1 - buf][comp, parity, side, half, rows_of(block), :] = new
            return tuple(totals)

        return sum(lax.fori_loop(0, blocks, body, (zero,) * 4, unroll=FINE_UNROLL))

    def back_rows(owner):
        return pl.ds(pl.multiple_of(owner * own_rows, SUB), own_rows)

    def back_columns(place):
        return pl.ds(pl.multiple_of(place * width, LANES), width)

    def send_back(comp):
        def send(peer):
            pltpu.make_async_remote_copy(
                patch_out.at[comp, back_rows(peer), :],
                coarse_out.at[comp, :, back_columns(gy)],
                back_send.at[0],
                back_recv.at[0],
                device_id={"gy": peer},
                device_id_type=MESH,
            ).start()

        each_step(send)
        coarse_out[comp, :, back_columns(gy)] = patch_out[comp, back_rows(gy), :]

    weave_a = jnp.where(lane % 2 == 0, lane // 2, lane // 2 + HALF)
    weave_b = jnp.where(lane % 2 == 0, lane // 2 + HALF, lane // 2)
    final = ITERS % 2

    def weave(comp):
        def body(block, carry):
            out = []
            for parity in range(2):
                for half in range(halves):
                    even = fine[final][comp, parity, 0, half, rows_of(block), :]
                    odd = fine[final][comp, parity, 1, half, rows_of(block), :]
                    odd = pltpu.roll(odd, HALF, 1)
                    at = pl.ds(block * 2 * SUB + parity, SUB, stride=2)
                    a = jnp.take_along_axis(jnp.where(half_lane, even, odd), weave_a, axis=1)
                    b = jnp.take_along_axis(jnp.where(half_lane, odd, even), weave_b, axis=1)
                    out.append((2 * half, at, a))
                    out.append((2 * half + 1, at, b))
            for tile, at, cells in out:
                fine_out[tile, comp, at, :] = cells
            return carry

        lax.fori_loop(0, blocks, body, 0, unroll=SPLIT_UNROLL)

    totals = [zero] * ITERS

    def on_coarse(sweep, comp):
        totals[sweep] = totals[sweep] + coarse_pass(sweep, comp)

    def on_fine(sweep, comp):
        totals[sweep] = totals[sweep] + fine_pass(sweep, comp)

    def place(comp):
        wait_moves(START + comp)
        place_start(comp)
        send_coarse(0, comp)

    def first_fine(comp):
        take_fine(0, comp)
        take_coarse(0, comp)
        on_fine(0, comp)
        send_fine(1, comp)

    def first_coarse(comp):
        wait_moves(KNOWN + comp)
        on_coarse(0, comp)
        send_coarse(1, comp)

    def second_coarse(comp):
        take_fine(1, comp)
        take_coarse(1, comp)
        on_coarse(1, comp)
        send_coarse(2, comp)

    def second_fine(comp):
        on_fine(1, comp)
        send_fine(2, comp)

    def last_coarse(comp):
        take_coarse(2, comp)
        on_coarse(2, comp)
        send_back(comp)

    def last_fine(comp):
        take_fine(2, comp)
        on_fine(2, comp)

    one_lane = lax.broadcasted_iota(jnp.int32, (1, LANES), 1)

    def gather_sum(sums, sweep):
        return jnp.where(one_lane == sweep, jnp.sum(totals[sweep]), sums)

    wait_bytes(own_planes, load_sem.at[3])
    send_moves(START)
    send_strips()
    wait_bytes(raw_start, load_sem.at[0])
    for comp in range(comps):
        send_fine_cols(0, comp)
    send_moves(START + 1)
    send_moves(START + 2)
    send_moves(MU)
    split_start(0)
    send_fine_rows(0, 0)
    split_start(1)
    send_fine_rows(0, 1)
    split_start(2)
    send_fine_rows(0, 2)
    wait_bytes(raw_mu, load_sem.at[1])
    lax.fori_loop(0, blocks, split_mu, 0, unroll=MU_UNROLL)
    wait_bytes(raw_known, load_sem.at[2])
    split_known(0)
    split_known(1)
    split_known(2)
    take_strips()
    place(0)
    send_moves(KNOWN)
    send_moves(KNOWN + 1)
    first_fine(0)
    place(1)
    send_moves(KNOWN + 2)
    first_fine(1)
    place(2)
    first_fine(2)
    wait_moves(MU)
    place_mu()
    first_coarse(0)
    first_coarse(1)
    first_coarse(2)
    second_coarse(0)
    second_fine(0)
    second_coarse(1)
    second_fine(1)
    last_coarse(0)
    second_coarse(2)
    second_fine(2)
    last_coarse(1)
    last_coarse(2)
    last_fine(0)
    last_fine(1)
    sums = jnp.zeros((1, LANES), jnp.float32)
    for sweep in range(ITERS - 1):
        sums = gather_sum(sums, sweep)
    last_fine(2)
    norm_all[me] = gather_sum(sums, ITERS - 1)
    each_device(
        lambda peer: pltpu.make_async_remote_copy(
            norm_all.at[me],
            norm_all.at[me],
            norm_send.at[0],
            norm_recv.at[0],
            device_id=peer,
            device_id_type=MESH,
        ).start()
    )
    weave(0)
    weave(1)
    weave(2)

    for direction in range(4):
        way = direction % 2

        @pl.when(inside(direction))
        def _():
            sent = (fine_row_send if direction < 2 else fine_col_send).at[:, :, way]
            wait_sent(sent, fine_send.at[direction])
            if direction < 2:
                wait_sent(row_send.at[:, :, way], halo_send.at[direction])

    wait_sent(strip_send.at[pl.ds(0, n_gy - 1)], edge_send.at[0])
    others = pl.ds(0, rows - own_rows)
    wait_sent(patch_start.at[:, others, :], move_send.at[0])
    wait_sent(patch_mu.at[others, :], move_send.at[1])
    wait_sent(patch_known.at[:, others, :], move_send.at[2])
    wait_sent(patch_out.at[:, others, :], back_send.at[0])
    rest = norm_all.at[pl.ds(0, count - 1)]
    wait_sent(rest, norm_send.at[0])
    wait_bytes(rest, norm_recv.at[0])
    whole = lax.fori_loop(
        0, count, lambda i, acc: acc + norm_all[i], jnp.zeros((1, LANES), jnp.float32)
    )
    norms_out[...] = jnp.broadcast_to(jnp.sqrt(whole / cells_total), norms_out.shape)
    wait_bytes(coarse_out.at[:, :, pl.ds(0, (n_gy - 1) * width)], back_recv.at[0])


def finish(fine_in, coarse_in, norms_in, fine_out, coarse_out, norms_out, held, sems):
    tiles = fine_in.shape[0]
    copies = [
        pltpu.make_async_copy(
            fine_in.at[tile], fine_out.at[:, :, pl.ds(tile * LANES, LANES)], sems.at[tile]
        )
        for tile in range(tiles)
    ]
    copies.append(pltpu.make_async_copy(coarse_in, coarse_out, sems.at[tiles]))
    for copy in copies:
        copy.start()
    for sweep in range(ITERS):
        held[sweep] = norms_in[0, sweep]
    copies.append(pltpu.make_async_copy(held, norms_out, sems.at[tiles + 1]))
    copies[-1].start()
    for copy in copies:
        copy.wait()


def on_device(n_gx, n_gy, fine_start, fine_known, fine_mu, coarse_start, coarse_known, coarse_mu):
    comps, fine_rows, fine_cols = fine_start.shape
    rows, width = fine_rows // 2, fine_cols // 2
    halves = width // LANES
    tiles = 2 * halves
    padded = rows + 2 * SUB
    row_pad = 1 << halves.bit_length()
    cells_total = 3.0 * (fine_mu.size + coarse_mu.size) * n_gx * n_gy
    f32 = jnp.float32
    dma = pltpu.SemaphoreType.DMA
    anywhere = pl.BlockSpec(memory_space=pl.ANY)
    in_vmem = pl.BlockSpec(memory_space=pltpu.VMEM)
    out_bytes = 4 * (fine_start.size + coarse_start.size + SUB * LANES)
    results = pl.pallas_call(
        functools.partial(kernel, n_gx, n_gy, cells_total),
        out_shape=(
            pltpu.VMEM((tiles, comps, fine_rows, LANES), f32),
            pltpu.VMEM(coarse_start.shape, f32),
            pltpu.VMEM((SUB, LANES), f32),
        ),
        in_specs=[pl.BlockSpec(memory_space=pltpu.HBM)] * 6,
        out_specs=(in_vmem,) * 3,
        scratch_shapes=[
            pltpu.VMEM((tiles, comps, fine_rows, LANES), f32),
            pltpu.VMEM((tiles, comps, fine_rows, LANES), f32),
            pltpu.VMEM((tiles, fine_rows, LANES), f32),
            pltpu.VMEM((comps, 2, 2, halves, padded, LANES), f32),
            pltpu.VMEM((comps, 2, 2, halves, padded, LANES), f32),
            pltpu.VMEM((comps, 2, 2, halves, rows, LANES), f32),
            pltpu.VMEM((2, 2, halves, rows, LANES), f32),
            pltpu.VMEM((2, 2, halves, rows, LANES), f32),
            pltpu.VMEM((comps, rows, width), f32),
            pltpu.VMEM((comps, rows, width), f32),
            pltpu.VMEM((rows, width), f32),
            pltpu.VMEM((rows, width), f32),
            pltpu.VMEM((comps, halves + 1, padded, LANES), f32),
            pltpu.VMEM((comps, halves + 1, padded, LANES), f32),
            pltpu.VMEM((comps, rows, width), f32),
            pltpu.VMEM((ITERS, comps, 2, tiles, LANES), f32),
            pltpu.VMEM((ITERS, comps, 2, tiles, LANES), f32),
            pltpu.VMEM((ITERS, comps, 2, 4, rows), f32),
            pltpu.VMEM((ITERS, comps, 2, 4, rows), f32),
            pltpu.VMEM((ITERS, comps, 2, row_pad, LANES), f32),
            pltpu.VMEM((ITERS, comps, 2, row_pad, LANES), f32),
            pltpu.VMEM((comps, rows, LANES), f32),
            pltpu.VMEM((2 * comps + 1,) + coarse_mu.shape, f32),
            pltpu.VMEM((n_gy, SUB, LANES), f32),
            pltpu.VMEM((n_gy, SUB, LANES), f32),
            pltpu.VMEM((comps, rows, LANES), f32),
            pltpu.VMEM((rows, LANES), f32),
            pltpu.VMEM((rows, LANES), f32),
            pltpu.VMEM((n_gx * n_gy, 1, LANES), f32),
            pltpu.VMEM((2 * tiles + 2 * row_pad + 8 * rows // LANES, 1, LANES), f32),
            dma((4,)),
            dma((3,)),
            dma((2 * comps + 1,)),
            dma((4,)),
            dma((ITERS, comps)),
            dma((2,)),
            dma((ITERS, comps)),
            dma((1,)),
            dma((1,)),
            dma((1,)),
            dma((1,)),
            dma((1,)),
            dma((1,)),
        ],
        compiler_params=pltpu.CompilerParams(
            collective_id=0,
            has_side_effects=True,
            vmem_limit_bytes=VMEM_BYTES - out_bytes - 2 * SUB * LANES * 4,
        ),
    )(fine_start, fine_known, fine_mu, coarse_start, coarse_known, coarse_mu)
    return pl.pallas_call(
        finish,
        out_shape=(
            jax.ShapeDtypeStruct(fine_start.shape, f32),
            jax.ShapeDtypeStruct(coarse_start.shape, f32),
            jax.ShapeDtypeStruct((ITERS,), f32),
        ),
        in_specs=[in_vmem] * 3,
        out_specs=(anywhere,) * 3,
        scratch_shapes=[pltpu.SMEM((ITERS,), f32), dma((tiles + 2,))],
        compiler_params=pltpu.CompilerParams(vmem_limit_bytes=2**20),
    )(*(pltpu.with_memory_space_constraint(result, pltpu.VMEM) for result in results))


def solution(mesh):
    n_gx, n_gy = mesh.shape["gx"], mesh.shape["gy"]
    return jax.shard_map(
        functools.partial(on_device, n_gx, n_gy),
        mesh=mesh,
        in_specs=(
            P(None, "gx", "gy"),
            P(None, "gx", "gy"),
            P("gx", "gy"),
            P(None, ("gx", "gy"), None),
            P(None, ("gx", "gy"), None),
            P(("gx", "gy"), None),
        ),
        out_specs=(P(None, "gx", "gy"), P(None, ("gx", "gy"), None), P()),
        check_vma=False,
    )
```

```python
import functools

import jax
import jax.numpy as jnp
from jax import lax
from jax.experimental import pallas as pl
from jax.experimental.pallas import tpu as pltpu
from jax.sharding import PartitionSpec as P

ITERS = 3
LANES = 128
SUB = 8
HALF = LANES // 2
VMEM_BYTES = 67043328
MESH = pl.DeviceIdType.MESH
DIRECTIONS = ((-1, 0), (1, 0), (0, -1), (0, 1))
QUARTER = LANES // 4
REACH = 4
FINE_UNROLL = 8
COARSE_UNROLL = 16
SPLIT_UNROLL = 8
MU_UNROLL = 8


def lane_index():
    return lax.broadcasted_iota(jnp.int32, (SUB, LANES), 1)


def roll_lanes(cells, shift):
    shift = shift % LANES
    return cells if shift == 0 else pltpu.roll(cells, shift, 1)


def beside_left(halves, halo):
    first = lane_index() == 0
    rolled = [roll_lanes(cells, 1) for cells in halves]
    return [jnp.where(first, before, own) for before, own in zip([halo] + rolled[:-1], rolled)]


def beside_right(halves, halo):
    last = lane_index() == LANES - 1
    rolled = [roll_lanes(cells, LANES - 1) for cells in halves]
    return [jnp.where(last, after, own) for own, after in zip(rolled, rolled[1:] + [halo])]


def from_left(ring):
    first = lane_index() == 0
    rolled = [roll_lanes(cells, 1) for cells in ring]
    return [jnp.where(first, rolled[at - 1], rolled[at]) for at in range(len(ring))]


def from_right(ring):
    last = lane_index() == LANES - 1
    rolled = [roll_lanes(cells, LANES - 1) for cells in ring]
    return [jnp.where(last, rolled[at + 1 - len(ring)], rolled[at]) for at in range(len(ring))]


def kernel(
    n_gx,
    n_gy,
    cells_total,
    fine_start,
    fine_known,
    fine_mu,
    coarse_start,
    coarse_known,
    coarse_mu,
    fine_out,
    coarse_out,
    norms_out,
    raw_start,
    raw_known,
    raw_mu,
    fine_a,
    fine_b,
    known,
    diag,
    inverse,
    patch_start,
    patch_known,
    patch_mu,
    patch_inverse,
    coarse_a,
    coarse_b,
    patch_out,
    fine_row_send,
    fine_row_recv,
    fine_col_send,
    fine_col_recv,
    row_send,
    row_recv,
    fine_halo,
    own_planes,
    strip_send,
    strip_recv,
    strip_known,
    strip_mu,
    strip_inverse,
    norm_all,
    tally,
    load_sem,
    move_send,
    move_recv,
    fine_send,
    fine_recv,
    halo_send,
    halo_recv,
    back_send,
    back_recv,
    norm_send,
    norm_recv,
    edge_send,
    edge_recv,
):
    gx = lax.axis_index("gx")
    gy = lax.axis_index("gy")
    me = gx * n_gy + gy
    count = n_gx * n_gy
    fine, coarse = (fine_a, fine_b), (coarse_a, coarse_b)
    comps, rows, width = patch_start.shape
    halves = width // LANES
    tiles = 2 * halves
    blocks = rows // SUB
    own_rows = coarse_start.shape[1]
    lane = lane_index()
    barrier = pltpu.get_barrier_semaphore()

    def wrap(at, size):
        return jnp.where(at < size, at, at - size)

    def each_device(action):
        for dy in reversed(range(n_gy)):
            for dx in range(n_gx):
                if dx or dy:
                    action({"gx": wrap(gx + dx, n_gx), "gy": wrap(gy + dy, n_gy)})

    each_device(
        lambda peer: pl.semaphore_signal(barrier, inc=1, device_id=peer, device_id_type=MESH)
    )

    pltpu.make_async_copy(coarse_start, own_planes.at[pl.ds(0, comps)], load_sem.at[3]).start()
    pltpu.make_async_copy(coarse_mu, own_planes.at[comps], load_sem.at[3]).start()
    pltpu.make_async_copy(
        coarse_known, own_planes.at[pl.ds(comps + 1, comps)], load_sem.at[3]
    ).start()

    loads = []
    for which, (source, target) in enumerate(
        ((fine_start, raw_start), (fine_mu, raw_mu), (fine_known, raw_known))
    ):
        for tile in range(tiles):
            at = pl.ds(tile * LANES, LANES)
            view = source.at[:, at] if len(source.shape) == 2 else source.at[:, :, at]
            loads.append(
                pltpu.make_async_copy(view, target.at[tile], load_sem.at[which])
            )
    for copy in loads:
        copy.start()

    def wait_bytes(ref, sem):
        pltpu.make_async_copy(ref, ref, sem).wait()

    def wait_sent(ref, sem):
        pltpu.make_async_remote_copy(
            ref, ref, sem, sem, device_id={"gy": gy}, device_id_type=MESH
        ).wait_send()

    def clear(edge, ref, way):
        @pl.when(edge)
        def _():
            for sweep in range(ITERS):
                for comp in range(comps):
                    at = ref.at[sweep, comp, way]
                    at[...] = jnp.zeros_like(at)

    for ref in (row_recv, fine_row_recv):
        clear(gx == 0, ref, 0)
        clear(gx == n_gx - 1, ref, 1)
    clear(gy == 0, fine_col_recv, 0)
    clear(gy == n_gy - 1, fine_col_recv, 1)
    row_send[...] = jnp.zeros_like(row_send)

    pl.semaphore_wait(barrier, count - 1)

    def inside(direction):
        dx, dy = DIRECTIONS[direction]
        checks = []
        if dx:
            checks.append(gx > 0 if dx < 0 else gx < n_gx - 1)
        if dy:
            checks.append(gy > 0 if dy < 0 else gy < n_gy - 1)
        return functools.reduce(jnp.logical_and, checks)

    START, MU, KNOWN = 0, comps, comps + 1

    def plane(item, owner, place):
        columns = pl.ds(pl.multiple_of(owner * width, LANES), width)
        lines = pl.ds(pl.multiple_of(place * own_rows, SUB), own_rows)
        source = own_planes.at[item, :, columns]
        if item == MU:
            return source, patch_mu.at[lines, :]
        if item < MU:
            return source, patch_start.at[item - START, lines, :]
        return source, patch_known.at[item - KNOWN, lines, :]

    def each_step(action):
        def body(step, carry):
            action(lax.rem(gy + step, n_gy))
            return carry

        lax.fori_loop(1, n_gy, body, 0)

    own_columns = pl.ds(pl.multiple_of(gy * width, LANES), width)

    def send_moves(item):
        kind = 0 if item < MU else 1 if item == MU else 2

        def send(peer):
            pltpu.make_async_remote_copy(
                *plane(item, peer, gy),
                move_send.at[kind],
                move_recv.at[item],
                device_id={"gy": peer},
                device_id_type=MESH,
            ).start()

        each_step(send)
        if item == MU:
            source = coarse_mu.at[:, own_columns]
        elif item < MU:
            source = coarse_start.at[item - START, :, own_columns]
        else:
            source = coarse_known.at[item - KNOWN, :, own_columns]
        pltpu.make_async_copy(source, plane(item, gy, gy)[1], move_recv.at[item]).start()

    def wait_moves(item):
        if item == MU:
            target = patch_mu
        elif item < MU:
            target = patch_start.at[item - START]
        else:
            target = patch_known.at[item - KNOWN]
        wait_bytes(target, move_recv.at[item])

    items = 2 * comps + 1
    half_lane = lane < HALF
    valid = jnp.where(half_lane, jnp.where(gy < n_gy - 1, 1, 0), jnp.where(gy > 0, 1, 0)) == 1
    own_tiles = own_rows // SUB
    share = LANES // own_tiles

    def strip_at(tile, item):
        return tile * share + 2 * REACH * item

    def send_strips():
        for owner in range(n_gy):
            cells = jnp.zeros((SUB, LANES), jnp.float32)
            for tile in range(own_tiles):
                lines = slice(tile * SUB, (tile + 1) * SUB)
                for item in range(items):
                    sides = []
                    for at in (halves * (owner + 1), halves * owner - 1):
                        at = at if 0 <= at < n_gy * halves else 0
                        sides.append(own_planes[item, lines, at * LANES : (at + 1) * LANES])
                    both = jnp.where(half_lane, *sides)
                    start = strip_at(tile, item)
                    here = jnp.logical_and(lane >= start, lane < start + 2 * REACH)
                    cells = jnp.where(here, roll_lanes(both, start + REACH), cells)
            strip_send[owner] = cells

        def send(peer):
            pltpu.make_async_remote_copy(
                strip_send.at[peer],
                strip_recv.at[gy],
                edge_send.at[0],
                edge_recv.at[0],
                device_id={"gy": peer},
                device_id_type=MESH,
            ).start()

        each_step(send)

    def take_strips():
        strip_recv[gy] = strip_send[gy]
        wait_bytes(strip_recv.at[pl.ds(0, n_gy - 1)], edge_recv.at[0])

        def body(owner, carry):
            cells = strip_recv[owner]
            for tile in range(own_tiles):
                block = owner * own_tiles + tile
                for item in range(items):
                    strip = roll_lanes(cells, -strip_at(tile, item) - REACH)
                    if item < MU:
                        coarse[0][item, halves, rows_of(block), :] = jnp.where(valid, strip, 0.0)
                    elif item == MU:
                        strip_mu[plain(block), :] = strip + 1.0
                        strip_inverse[plain(block), :] = 1.0 / (strip + 1.0)
                    else:
                        strip_known[item - KNOWN, plain(block), :] = strip
            return carry

        lax.fori_loop(0, n_gy, body, 0, unroll=2)

    evens_first = jnp.where(half_lane, 2 * lane, 2 * lane - LANES + 1)
    odds_first = jnp.where(half_lane, 2 * lane + 1, 2 * lane - LANES)

    def split_columns(a, b):
        a = jnp.take_along_axis(a, evens_first, axis=1)
        b = jnp.take_along_axis(b, odds_first, axis=1)
        return (
            jnp.where(half_lane, a, b),
            pltpu.roll(jnp.where(half_lane, b, a), HALF, 1),
        )

    def rows_of(block, shift=0):
        if shift == 0:
            return pl.ds(pl.multiple_of(block * SUB + SUB, SUB), SUB)
        return pl.ds(block * SUB + SUB + shift, SUB)

    def plain(block):
        return pl.ds(pl.multiple_of(block * SUB, SUB), SUB)

    inner = pl.ds(SUB, rows)

    def split_field(raw, comp, put):
        def body(block, carry):
            out = []
            for parity in range(2):
                for half in range(halves):
                    at = pl.ds(block * 2 * SUB + parity, SUB, stride=2)
                    both = split_columns(raw[2 * half, comp, at, :], raw[2 * half + 1, comp, at, :])
                    out.append((parity, half, both))
            for parity, half, both in out:
                put(parity, 0, half, block, both[0])
                put(parity, 1, half, block, both[1])
            return carry

        lax.fori_loop(0, blocks, body, 0, unroll=SPLIT_UNROLL)

    def split_start(comp):
        def put(parity, side, half, block, cells):
            fine[0][comp, parity, side, half, rows_of(block), :] = cells

        split_field(raw_start, comp, put)

    def split_known(comp):
        def put(parity, side, half, block, cells):
            known[comp, parity, side, half, plain(block), :] = cells

        split_field(raw_known, comp, put)

    def split_mu(block, carry):
        out = []
        for parity in range(2):
            for half in range(halves):
                at = pl.ds(block * 2 * SUB + parity, SUB, stride=2)
                both = split_columns(raw_mu[2 * half, at, :], raw_mu[2 * half + 1, at, :])
                for side in range(2):
                    total = both[side] + 1.0
                    out.append((parity, side, half, total, 1.0 / total))
        for parity, side, half, total, reciprocal in out:
            diag[parity, side, half, plain(block), :] = total
            inverse[parity, side, half, plain(block), :] = reciprocal
        return carry

    def place_mu():
        def body(block, carry):
            total = patch_mu[plain(block), :] + 1.0
            patch_mu[plain(block), :] = total
            patch_inverse[plain(block), :] = 1.0 / total
            return carry

        lax.fori_loop(0, blocks, body, 0, unroll=4)

    def place_start(comp):
        for half in range(halves):
            coarse[0][comp, half, inner, :] = patch_start[
                comp, :, half * LANES : (half + 1) * LANES
            ]

    def message(direction, source, target, send, recv):
        dx, dy = DIRECTIONS[direction]

        @pl.when(inside(direction))
        def _():
            pltpu.make_async_remote_copy(
                source,
                target,
                send.at[direction],
                recv,
                device_id={"gx": gx + dx, "gy": gy + dy},
                device_id_type=MESH,
            ).start()

    edge_x = jnp.logical_or(gx == 0, gx == n_gx - 1)
    edge_y = jnp.logical_or(gy == 0, gy == n_gy - 1)
    sides_x = ((1, edge_x), (2, jnp.logical_not(edge_x)))
    sides_y = ((1, edge_y), (2, jnp.logical_not(edge_y)))

    all_lanes = lax.broadcasted_iota(jnp.int32, (rows, LANES), 1)
    low = all_lanes < HALF
    middle = jnp.logical_and(all_lanes >= HALF, all_lanes < HALF + QUARTER)
    middle = jnp.logical_or(middle, jnp.logical_and(all_lanes >= HALF - SUB, all_lanes < HALF))
    beside = jnp.logical_and(all_lanes >= QUARTER - REACH, all_lanes < QUARTER + REACH)

    def send_fine_cols(sweep, comp):
        buf = sweep % 2
        parts, sums = [], []
        for parity in range(2):
            if sweep == 0:
                at = pl.ds(parity, rows, stride=2)
                ends = [raw_start[0, comp, at, :], raw_start[tiles - 1, comp, at, :]]
                sums.append(ends)
            else:
                ends = [
                    fine[buf][comp, parity, side, half, inner, :]
                    for side, half in ((0, 0), (1, halves - 1))
                ]
                others = [
                    fine[buf][comp, parity, 1 - side, half, inner, :]
                    for side, half in ((0, 0), (1, halves - 1))
                ]
                sums.append([a + b for a, b in zip(ends, others)])
            parts.append(jnp.where(low, *ends))
        total = jnp.where(low, sums[0][0] + sums[1][0], sums[0][1] + sums[1][1])
        pitch = 1
        if sweep == 0:
            total = total + pltpu.roll(total, LANES - 1, 1)
            pitch = 2
        mixed = jnp.where(middle, pltpu.roll(parts[1], HALF, 1), parts[0])
        turned = jnp.where(beside, pltpu.roll(total, QUARTER, 1), mixed).T
        first = (0, HALF, QUARTER, QUARTER + pitch)
        last = (LANES - 1, HALF - 1, QUARTER - pitch, QUARTER - 2 * pitch)
        for way, lines in enumerate((first, last)):
            for at, line in enumerate(lines):
                fine_col_send[sweep, comp, way, at : at + 1, :] = turned[line : line + 1]
            message(
                2 + way,
                fine_col_send.at[sweep, comp, way],
                fine_col_recv.at[sweep, comp, 1 - way],
                fine_send,
                fine_recv.at[sweep, comp],
            )

    def send_fine_rows(sweep, comp):
        buf = sweep % 2
        for way, line in enumerate((SUB, SUB + rows - 1)):
            for half in range(halves):
                for side in range(2):
                    at = 2 * half + side
                    fine_row_send[sweep, comp, way, at : at + 1, :] = fine[buf][
                        comp, way, side, half, line : line + 1, :
                    ]
            message(
                way,
                fine_row_send.at[sweep, comp, way],
                fine_row_recv.at[sweep, comp, 1 - way],
                fine_send,
                fine_recv.at[sweep, comp],
            )

    def send_fine(sweep, comp):
        send_fine_cols(sweep, comp)
        send_fine_rows(sweep, comp)

    line_at = lax.broadcasted_iota(jnp.int32, (SUB, rows), 0)

    def take_fine(sweep, comp):
        buf = sweep % 2
        for count_x, at_x in sides_x:
            for count_y, at_y in sides_y:

                @pl.when(jnp.logical_and(at_x, at_y))
                def _():
                    units = tiles * count_x + 4 * rows // LANES * count_y
                    wait_bytes(tally.at[pl.ds(0, units)], fine_recv.at[sweep, comp])

        for half in range(halves):
            for side in range(2):
                at = 2 * half + side
                fine[buf][comp, 1, side, half, SUB - 1 : SUB, :] = fine_row_recv[
                    sweep, comp, 0, at : at + 1, :
                ]
                fine[buf][comp, 0, side, half, SUB + rows : SUB + rows + 1, :] = fine_row_recv[
                    sweep, comp, 1, at : at + 1, :
                ]
        left, right = (
            [
                jnp.broadcast_to(fine_col_recv[sweep, comp, way, at : at + 1, :], (SUB, rows))
                for at in range(4)
            ]
            for way in range(2)
        )
        near_left = jnp.where(line_at == SUB - 1, left[2], left[3])
        near_right = jnp.where(line_at == 0, right[2], right[3])
        turned = jnp.concatenate(
            [left[0]] * 3
            + [near_left, near_right]
            + [right[1]] * 3
            + [left[1]] * 4
            + [right[0]] * 4,
            axis=0,
        )
        fine_halo[comp] = turned.T

    def send_coarse(sweep, comp):
        buf = sweep % 2
        for way, line in enumerate((SUB, SUB + rows - 1)):
            for tile in range(halves + 1):
                row_send[sweep, comp, way, tile : tile + 1, :] = coarse[buf][
                    comp, tile, line : line + 1, :
                ]
            message(
                way,
                row_send.at[sweep, comp, way],
                row_recv.at[sweep, comp, 1 - way],
                halo_send,
                halo_recv.at[sweep, comp],
            )

    def take_coarse(sweep, comp):
        buf = sweep % 2
        for count_x, at_x in sides_x:

            @pl.when(at_x)
            def _():
                units = row_send.shape[3] * count_x
                wait_bytes(tally.at[pl.ds(0, units)], halo_recv.at[sweep, comp])

        for way, line in enumerate((SUB - 1, SUB + rows)):
            for tile in range(halves + 1):
                coarse[buf][comp, tile, line : line + 1, :] = row_recv[
                    sweep, comp, way, tile : tile + 1, :
                ]

    zero = jnp.zeros((SUB, LANES), jnp.float32)

    def coarse_pass(sweep, comp):
        buf = sweep % 2
        last = sweep == ITERS - 1

        def body(block, totals):
            totals = list(totals)
            lines = plain(block)
            out = []
            ring = [coarse[buf][comp, tile, rows_of(block), :] for tile in range(halves + 1)]
            lefts, rights = from_left(ring), from_right(ring)
            for tile in range(halves if last else halves + 1):
                columns = slice(tile * LANES, (tile + 1) * LANES)
                near = (
                    coarse[buf][comp, tile, rows_of(block, 1), :]
                    + coarse[buf][comp, tile, rows_of(block, -1), :]
                    + rights[tile]
                    + lefts[tile]
                )
                if tile < halves:
                    below = (
                        fine[buf][comp, 0, 0, tile, rows_of(block), :]
                        + fine[buf][comp, 1, 0, tile, rows_of(block), :]
                        + fine[buf][comp, 0, 1, tile, rows_of(block), :]
                        + fine[buf][comp, 1, 1, tile, rows_of(block), :]
                    )
                    given = patch_known[comp, lines, columns]
                    scale, reciprocal = patch_mu[lines, columns], patch_inverse[lines, columns]
                else:
                    below = roll_lanes(fine_halo[comp, lines, :], -QUARTER)
                    given = strip_known[comp, lines, :]
                    scale, reciprocal = strip_mu[lines, :], strip_inverse[lines, :]
                res = given + 0.25 * near + 0.125 * below - scale * ring[tile]
                new = ring[tile] + res * reciprocal
                if tile < halves:
                    totals[tile % 2] = totals[tile % 2] + res * res
                else:
                    new = jnp.where(valid, new, 0.0)
                out.append((tile, new))
            for tile, new in out:
                if last:
                    patch_out[comp, lines, tile * LANES : (tile + 1) * LANES] = new
                else:
                    coarse[1 - buf][comp, tile, rows_of(block), :] = new
            return tuple(totals)

        return sum(lax.fori_loop(0, blocks, body, (zero,) * 2, unroll=COARSE_UNROLL))

    def fine_pass(sweep, comp):
        buf = sweep % 2

        def body(block, totals):
            totals = list(totals)
            out = []
            mid = [coarse[buf][comp, tile, rows_of(block), :] for tile in range(halves + 1)]
            fine_edges = fine_halo[comp, plain(block), :]
            for parity in range(2):
                shift = 1 if parity else -1
                line = [
                    0.75 * mid[tile] + 0.25 * coarse[buf][comp, tile, rows_of(block, shift), :]
                    for tile in range(halves + 1)
                ]
                line_left, line_right = from_left(line), from_right(line)
                edge = roll_lanes(fine_edges, HALF) if parity else fine_edges
                evens, odds = (
                    [fine[buf][comp, parity, side, half, rows_of(block), :] for half in range(halves)]
                    for side in range(2)
                )
                before, after = beside_left(odds, edge), beside_right(evens, edge)
                for half in range(halves):
                    for side in range(2):
                        own = odds[half] if side else evens[half]
                        lateral = evens[half] + after[half] if side else odds[half] + before[half]
                        near = (
                            fine[buf][comp, 1 - parity, side, half, rows_of(block), :]
                            + fine[buf][comp, 1 - parity, side, half, rows_of(block, shift), :]
                            + lateral
                        )
                        spread = 0.75 * line[half] + 0.25 * (
                            line_right[half] if side else line_left[half]
                        )
                        res = (
                            known[comp, parity, side, half, plain(block), :]
                            + 0.25 * near
                            + 0.5 * spread
                            - diag[parity, side, half, plain(block), :] * own
                        )
                        at = 2 * parity + side
                        totals[at] = totals[at] + res * res
                        new = own + res * inverse[parity, side, half, plain(block), :]
                        out.append((parity, side, half, new))
            for parity, side, half, new in out:
                fine[1 - buf][comp, parity, side, half, rows_of(block), :] = new
            return tuple(totals)

        return sum(lax.fori_loop(0, blocks, body, (zero,) * 4, unroll=FINE_UNROLL))

    def back_rows(owner):
        return pl.ds(pl.multiple_of(owner * own_rows, SUB), own_rows)

    def back_columns(place):
        return pl.ds(pl.multiple_of(place * width, LANES), width)

    def send_back(comp):
        def send(peer):
            pltpu.make_async_remote_copy(
                patch_out.at[comp, back_rows(peer), :],
                coarse_out.at[comp, :, back_columns(gy)],
                back_send.at[0],
                back_recv.at[0],
                device_id={"gy": peer},
                device_id_type=MESH,
            ).start()

        each_step(send)
        coarse_out[comp, :, back_columns(gy)] = patch_out[comp, back_rows(gy), :]

    weave_a = jnp.where(lane % 2 == 0, lane // 2, lane // 2 + HALF)
    weave_b = jnp.where(lane % 2 == 0, lane // 2 + HALF, lane // 2)
    final = ITERS % 2

    def weave(comp):
        def body(block, carry):
            out = []
            for parity in range(2):
                for half in range(halves):
                    even = fine[final][comp, parity, 0, half, rows_of(block), :]
                    odd = fine[final][comp, parity, 1, half, rows_of(block), :]
                    odd = pltpu.roll(odd, HALF, 1)
                    at = pl.ds(block * 2 * SUB + parity, SUB, stride=2)
                    a = jnp.take_along_axis(jnp.where(half_lane, even, odd), weave_a, axis=1)
                    b = jnp.take_along_axis(jnp.where(half_lane, odd, even), weave_b, axis=1)
                    out.append((2 * half, at, a))
                    out.append((2 * half + 1, at, b))
            for tile, at, cells in out:
                fine_out[tile, comp, at, :] = cells
            return carry

        lax.fori_loop(0, blocks, body, 0, unroll=SPLIT_UNROLL)

    totals = [zero] * ITERS

    def on_coarse(sweep, comp):
        totals[sweep] = totals[sweep] + coarse_pass(sweep, comp)

    def on_fine(sweep, comp):
        totals[sweep] = totals[sweep] + fine_pass(sweep, comp)

    def place(comp):
        wait_moves(START + comp)
        place_start(comp)
        send_coarse(0, comp)

    def first_fine(comp):
        take_fine(0, comp)
        take_coarse(0, comp)
        on_fine(0, comp)
        send_fine(1, comp)

    def first_coarse(comp):
        wait_moves(KNOWN + comp)
        on_coarse(0, comp)
        send_coarse(1, comp)

    def second_coarse(comp):
        take_fine(1, comp)
        take_coarse(1, comp)
        on_coarse(1, comp)
        send_coarse(2, comp)

    def second_fine(comp):
        on_fine(1, comp)
        send_fine(2, comp)

    def last_coarse(comp):
        take_coarse(2, comp)
        on_coarse(2, comp)
        send_back(comp)

    def last_fine(comp):
        take_fine(2, comp)
        on_fine(2, comp)

    one_lane = lax.broadcasted_iota(jnp.int32, (1, LANES), 1)

    def gather_sum(sums, sweep):
        return jnp.where(one_lane == sweep, jnp.sum(totals[sweep]), sums)

    wait_bytes(own_planes, load_sem.at[3])
    send_moves(START)
    send_strips()
    wait_bytes(raw_start, load_sem.at[0])
    for comp in range(comps):
        send_fine_cols(0, comp)
    send_moves(START + 1)
    send_moves(START + 2)
    send_moves(MU)
    split_start(0)
    send_fine_rows(0, 0)
    split_start(1)
    send_fine_rows(0, 1)
    split_start(2)
    send_fine_rows(0, 2)
    wait_bytes(raw_mu, load_sem.at[1])
    lax.fori_loop(0, blocks, split_mu, 0, unroll=MU_UNROLL)
    wait_bytes(raw_known, load_sem.at[2])
    split_known(0)
    split_known(1)
    split_known(2)
    take_strips()
    place(0)
    send_moves(KNOWN)
    send_moves(KNOWN + 1)
    first_fine(0)
    place(1)
    send_moves(KNOWN + 2)
    first_fine(1)
    place(2)
    first_fine(2)
    wait_moves(MU)
    place_mu()
    first_coarse(0)
    first_coarse(1)
    first_coarse(2)
    second_coarse(0)
    second_fine(0)
    second_coarse(1)
    second_fine(1)
    last_coarse(0)
    second_coarse(2)
    second_fine(2)
    last_coarse(1)
    last_coarse(2)
    last_fine(0)
    last_fine(1)
    sums = jnp.zeros((1, LANES), jnp.float32)
    for sweep in range(ITERS - 1):
        sums = gather_sum(sums, sweep)
    last_fine(2)
    norm_all[me] = gather_sum(sums, ITERS - 1)
    each_device(
        lambda peer: pltpu.make_async_remote_copy(
            norm_all.at[me],
            norm_all.at[me],
            norm_send.at[0],
            norm_recv.at[0],
            device_id=peer,
            device_id_type=MESH,
        ).start()
    )
    weave(0)
    weave(1)
    weave(2)

    for direction in range(4):
        way = direction % 2

        @pl.when(inside(direction))
        def _():
            sent = (fine_row_send if direction < 2 else fine_col_send).at[:, :, way]
            wait_sent(sent, fine_send.at[direction])
            if direction < 2:
                wait_sent(row_send.at[:, :, way], halo_send.at[direction])

    wait_sent(strip_send.at[pl.ds(0, n_gy - 1)], edge_send.at[0])
    others = pl.ds(0, rows - own_rows)
    wait_sent(patch_start.at[:, others, :], move_send.at[0])
    wait_sent(patch_mu.at[others, :], move_send.at[1])
    wait_sent(patch_known.at[:, others, :], move_send.at[2])
    wait_sent(patch_out.at[:, others, :], back_send.at[0])
    rest = norm_all.at[pl.ds(0, count - 1)]
    wait_sent(rest, norm_send.at[0])
    wait_bytes(rest, norm_recv.at[0])
    whole = lax.fori_loop(
        0, count, lambda i, acc: acc + norm_all[i], jnp.zeros((1, LANES), jnp.float32)
    )
    norms_out[...] = jnp.broadcast_to(jnp.sqrt(whole / cells_total), norms_out.shape)
    wait_bytes(coarse_out.at[:, :, pl.ds(0, (n_gy - 1) * width)], back_recv.at[0])


def finish(fine_in, coarse_in, norms_in, fine_out, coarse_out, norms_out, held, sems):
    tiles = fine_in.shape[0]
    copies = [
        pltpu.make_async_copy(
            fine_in.at[tile], fine_out.at[:, :, pl.ds(tile * LANES, LANES)], sems.at[tile]
        )
        for tile in range(tiles)
    ]
    copies.append(pltpu.make_async_copy(coarse_in, coarse_out, sems.at[tiles]))
    for copy in copies:
        copy.start()
    for sweep in range(ITERS):
        held[sweep] = norms_in[0, sweep]
    copies.append(pltpu.make_async_copy(held, norms_out, sems.at[tiles + 1]))
    copies[-1].start()
    for copy in copies:
        copy.wait()


def on_device(n_gx, n_gy, fine_start, fine_known, fine_mu, coarse_start, coarse_known, coarse_mu):
    comps, fine_rows, fine_cols = fine_start.shape
    rows, width = fine_rows // 2, fine_cols // 2
    halves = width // LANES
    tiles = 2 * halves
    padded = rows + 2 * SUB
    row_pad = 1 << halves.bit_length()
    cells_total = 3.0 * (fine_mu.size + coarse_mu.size) * n_gx * n_gy
    f32 = jnp.float32
    dma = pltpu.SemaphoreType.DMA
    anywhere = pl.BlockSpec(memory_space=pl.ANY)
    in_vmem = pl.BlockSpec(memory_space=pltpu.VMEM)
    out_bytes = 4 * (fine_start.size + coarse_start.size + SUB * LANES)
    results = pl.pallas_call(
        functools.partial(kernel, n_gx, n_gy, cells_total),
        out_shape=(
            pltpu.VMEM((tiles, comps, fine_rows, LANES), f32),
            pltpu.VMEM(coarse_start.shape, f32),
            pltpu.VMEM((SUB, LANES), f32),
        ),
        in_specs=[pl.BlockSpec(memory_space=pltpu.HBM)] * 6,
        out_specs=(in_vmem,) * 3,
        scratch_shapes=[
            pltpu.VMEM((tiles, comps, fine_rows, LANES), f32),
            pltpu.VMEM((tiles, comps, fine_rows, LANES), f32),
            pltpu.VMEM((tiles, fine_rows, LANES), f32),
            pltpu.VMEM((comps, 2, 2, halves, padded, LANES), f32),
            pltpu.VMEM((comps, 2, 2, halves, padded, LANES), f32),
            pltpu.VMEM((comps, 2, 2, halves, rows, LANES), f32),
            pltpu.VMEM((2, 2, halves, rows, LANES), f32),
            pltpu.VMEM((2, 2, halves, rows, LANES), f32),
            pltpu.VMEM((comps, rows, width), f32),
            pltpu.VMEM((comps, rows, width), f32),
            pltpu.VMEM((rows, width), f32),
            pltpu.VMEM((rows, width), f32),
            pltpu.VMEM((comps, halves + 1, padded, LANES), f32),
            pltpu.VMEM((comps, halves + 1, padded, LANES), f32),
            pltpu.VMEM((comps, rows, width), f32),
            pltpu.VMEM((ITERS, comps, 2, tiles, LANES), f32),
            pltpu.VMEM((ITERS, comps, 2, tiles, LANES), f32),
            pltpu.VMEM((ITERS, comps, 2, 4, rows), f32),
            pltpu.VMEM((ITERS, comps, 2, 4, rows), f32),
            pltpu.VMEM((ITERS, comps, 2, row_pad, LANES), f32),
            pltpu.VMEM((ITERS, comps, 2, row_pad, LANES), f32),
            pltpu.VMEM((comps, rows, LANES), f32),
            pltpu.VMEM((2 * comps + 1,) + coarse_mu.shape, f32),
            pltpu.VMEM((n_gy, SUB, LANES), f32),
            pltpu.VMEM((n_gy, SUB, LANES), f32),
            pltpu.VMEM((comps, rows, LANES), f32),
            pltpu.VMEM((rows, LANES), f32),
            pltpu.VMEM((rows, LANES), f32),
            pltpu.VMEM((n_gx * n_gy, 1, LANES), f32),
            pltpu.VMEM((2 * tiles + 2 * row_pad + 8 * rows // LANES, 1, LANES), f32),
            dma((4,)),
            dma((3,)),
            dma((2 * comps + 1,)),
            dma((4,)),
            dma((ITERS, comps)),
            dma((2,)),
            dma((ITERS, comps)),
            dma((1,)),
            dma((1,)),
            dma((1,)),
            dma((1,)),
            dma((1,)),
            dma((1,)),
        ],
        compiler_params=pltpu.CompilerParams(
            collective_id=0,
            has_side_effects=True,
            vmem_limit_bytes=VMEM_BYTES - out_bytes - 2 * SUB * LANES * 4,
        ),
    )(fine_start, fine_known, fine_mu, coarse_start, coarse_known, coarse_mu)
    return pl.pallas_call(
        finish,
        out_shape=(
            jax.ShapeDtypeStruct(fine_start.shape, f32),
            jax.ShapeDtypeStruct(coarse_start.shape, f32),
            jax.ShapeDtypeStruct((ITERS,), f32),
        ),
        in_specs=[in_vmem] * 3,
        out_specs=(anywhere,) * 3,
        scratch_shapes=[pltpu.SMEM((ITERS,), f32), dma((tiles + 2,))],
        compiler_params=pltpu.CompilerParams(vmem_limit_bytes=2**20),
    )(*(pltpu.with_memory_space_constraint(result, pltpu.VMEM) for result in results))


def solution(mesh):
    n_gx, n_gy = mesh.shape["gx"], mesh.shape["gy"]
    return jax.shard_map(
        functools.partial(on_device, n_gx, n_gy),
        mesh=mesh,
        in_specs=(
            P(None, "gx", "gy"),
            P(None, "gx", "gy"),
            P("gx", "gy"),
            P(None, ("gx", "gy"), None),
            P(None, ("gx", "gy"), None),
            P(("gx", "gy"), None),
        ),
        out_specs=(P(None, "gx", "gy"), P(None, ("gx", "gy"), None), P()),
        check_vma=False,
    )
```
